32 devices in a mesh: dp: 4 (over y, x), seq: 8 (over z, core).
Axes of the slice: x: 2, y: 2, z: 4, core: 2. Of those that a mesh axis runs over, the one named last changes fastest.
Arguments:
- queries: bfloat16 [4, 1024, 2048], P('dp', 'seq'), may hold values from -6 to 6
- key_vectors: bfloat16 [4, 1024, 2048], P('dp', 'seq'), may hold values from -6 to 6
- values: bfloat16 [4, 1024, 2048], P('dp', 'seq'), may hold values from -6 to 6
- out_grad: bfloat16 [4, 1024, 2048], P('dp', 'seq'), may hold values from -6 to 6
- inputs: bfloat16 [4, 1024, 2048], P('dp', 'seq'), may hold values from -6 to 6
Outputs:
- query_grad: bfloat16 [4, 1024, 2048], P('dp', 'seq')
- key_grad: bfloat16 [4, 1024, 2048], P('dp', 'seq')
- value_grad: bfloat16 [4, 1024, 2048], P('dp', 'seq')
- weight_grad: float32 [2048, 2048], P('dp', 'seq')
The draws below stay inside these ranges and needn't reach their ends.
All inputs are finite; a program needn't handle non-finite values.
Results may differ from the reference program's by a relative error of at most 0.025.
Values may be sent and summed in bfloat16 or wider, within the bound.
No kernel may reach another device: no remote copies, remote signals or barrier semaphores. Data moves between devices by JAX's collectives and lax.ppermute only.
A program may use at most 128 MiB of HBM per device.

```python
import jax
import jax.numpy as jnp
from jax import lax

DM = 2048
H = 16
HD = 128
HW = 2048
SEQ = 1024
DOCLEN = 256
SAMPLES = 4


def base_draw(key, salt):
    base_key = jax.random.fold_in(key, salt)
    return jnp.clip(jax.random.normal(base_key, (SAMPLES, SEQ, H * HD), jnp.float32), -6.0, 6.0)


def draw_queries(key, part):
    base = base_draw(key, 7)
    return base.astype(jnp.bfloat16)


def draw_key_vectors(key, part):
    base = base_draw(key, 9)
    return base.astype(jnp.bfloat16)


def raised(values, rng, source, target, shards_of, factor):
    owner, partner = [(jnp.arange(values.shape[dim]) // (values.shape[dim] // shards_of)).reshape([-1 if axis == dim else 1 for axis in range(values.ndim)]) for dim in (source, target)]
    chosen = jax.random.permutation(rng, shards_of)[partner]
    strong = (owner == chosen) | (owner == (partner + shards_of // 2) % shards_of)
    return jnp.where(strong, factor * values, values)


def level_of(key, extent, cuts, smallest, largest):
    def one(dim, parts):
        heights = jax.random.uniform(jax.random.fold_in(jax.random.fold_in(key, 6), dim), (parts,), jnp.float32, smallest / len(cuts), largest / len(cuts))
        return jnp.repeat(jnp.exp(heights), extent[dim] // parts).reshape((-1,) + (1,) * (len(extent) - dim - 1))

    gain = one(*cuts[0])
    for cut in cuts[1:]:
        gain = gain * one(*cut)
    return gain


def centred(own_key, dims, width, reach, shards=(), kind=jnp.bfloat16):
    loudness = level_of(own_key, dims, shards, -0.22, 0.18) if shards else 1.0
    drawn = jax.random.normal(own_key, dims, jnp.float32) * width * loudness
    return jnp.minimum(jnp.maximum(drawn, -reach), reach).astype(kind)


def heavy_noise(stream_key, extent, deviation, reach, cuts, heavy, held_as=jnp.bfloat16):
    values = deviation * jax.random.normal(stream_key, extent, jnp.float32)
    if cuts:
        values = values * level_of(stream_key, extent, cuts, -0.22, 0.18)
    return jnp.clip(raised(values, jax.random.fold_in(stream_key, 3), *heavy), -reach, reach).astype(held_as)


def setup_inputs(seed: int = 0) -> dict:
    key_of = jax.random.split(jax.random.key(seed), 6)
    return {
        "queries": draw_queries(jax.random.fold_in(key_of[5], 71), 0),
        "key_vectors": draw_key_vectors(jax.random.fold_in(key_of[5], 71), 0),
        "values": centred(key_of[2], (SAMPLES, SEQ, HW), 1.0, 6.0, ((0, 4), (1, 8))),
        "out_grad": centred(key_of[3], (SAMPLES, SEQ, HW), 1.0, 6.0, ((0, 4), (1, 8))),
        "inputs": heavy_noise(key_of[4], (SAMPLES, SEQ, DM), 1.0, 6.0, ((0, 4), (1, 8)), (0, 2, 4, 2.0)),
    }


def head_grads(items):
    q_head, k_head, v_head, g_head = items
    q_full = q_head.astype(jnp.float32)
    k_full = k_head.astype(jnp.float32)
    v_full = v_head.astype(jnp.float32)
    g_full = g_head.astype(jnp.float32)
    scale = HD ** -0.5
    scores = jnp.dot(q_full, k_full.T, precision=lax.Precision.HIGHEST, preferred_element_type=jnp.float32) * scale
    position = jnp.arange(SEQ, dtype=jnp.int32)
    document = position // DOCLEN
    visible = (position[None, :] <= position[:, None]) & (document[None, :] == document[:, None])
    scores = jnp.where(visible, scores, -jnp.inf)
    top = jnp.max(scores, axis=1, keepdims=True)
    weights = jnp.exp(scores - top)
    probs = weights / jnp.sum(weights, axis=1, keepdims=True)
    probs_low = probs.astype(jnp.bfloat16).astype(jnp.float32)
    dprob = jnp.dot(g_full, v_full.T, precision=lax.Precision.HIGHEST, preferred_element_type=jnp.float32)
    delta = jnp.sum(probs * dprob, axis=1, keepdims=True)
    dscore = (probs * (dprob - delta) * scale).astype(jnp.bfloat16).astype(jnp.float32)
    query_grad = jnp.dot(dscore, k_full, precision=lax.Precision.HIGHEST, preferred_element_type=jnp.float32).astype(jnp.bfloat16)

    def parity_sum(left, right):
        even_part = jnp.dot(left[0::2].T, right[0::2], precision=lax.Precision.HIGHEST, preferred_element_type=jnp.float32).astype(jnp.bfloat16)
        odd_part = jnp.dot(left[1::2].T, right[1::2], precision=lax.Precision.HIGHEST, preferred_element_type=jnp.float32).astype(jnp.bfloat16)
        return (even_part.astype(jnp.float32) + odd_part.astype(jnp.float32)).astype(jnp.bfloat16)

    key_grad = parity_sum(dscore, q_full)
    value_grad = parity_sum(probs_low, g_full)
    return query_grad, key_grad, value_grad


def split_heads(array):
    return array.reshape(SEQ, H, HD).transpose(1, 0, 2)


def join_heads(array):
    return array.transpose(1, 0, 2).reshape(SEQ, H * HD)


def sample_grads(items):
    q_all, k_all, v_all, g_all = items
    grads = lax.map(head_grads, (split_heads(q_all), split_heads(k_all), split_heads(v_all), split_heads(g_all)))
    return join_heads(grads[0]), join_heads(grads[1]), join_heads(grads[2])


def reference(queries, key_vectors, values, out_grad, inputs):
    query_grad, key_grad, value_grad = lax.map(sample_grads, (queries, key_vectors, values, out_grad))
    weight_grad = jnp.einsum("std,sth->dh", inputs.astype(jnp.float32), value_grad.astype(jnp.float32), precision=lax.Precision.HIGHEST)
    return query_grad, key_grad, value_grad, weight_grad
```

```python
import jax
import jax.numpy as jnp
from jax import lax
from jax.experimental import pallas as pl
from jax.experimental.pallas import tpu as pltpu
from jax.sharding import PartitionSpec as P

HD = 128


def partner(value, axis, apart):
    return lax.ppermute(value, axis, [(i, i ^ 1 << apart) for i in range(lax.axis_size(axis))])


def body(queries, key_vectors, values, out_grad, inputs):
    seq_count = lax.axis_size("seq")
    groups = seq_count // 2
    parity = lax.axis_index("seq") % 2
    is_even = parity == 0
    tok_rows = queries.shape[1]
    half_rows = tok_rows // 2
    width = queries.shape[2]
    group_width = 2 * width // seq_count
    heads_here = group_width // HD
    model_width = inputs.shape[2]
    own_rows = seq_count * half_rows
    length = 2 * own_rows
    doc_rows = own_rows // 4
    block_rows = min(doc_rows, max(256, length // 16))
    block_count = own_rows // block_rows
    scale = HD ** (-0.5)

    def to_heads(array):
        return (
            array[0]
            .reshape(half_rows, 2, groups, group_width)
            .transpose(0, 2, 1, 3)
            .reshape(half_rows, seq_count, group_width)
        )

    moved = (
        lax.all_to_all(to_heads(queries), "seq", split_axis=1, concat_axis=0, tiled=True),
        lax.all_to_all(to_heads(key_vectors), "seq", split_axis=1, concat_axis=0, tiled=True),
        lax.all_to_all(to_heads(values), "seq", split_axis=1, concat_axis=0, tiled=True),
        lax.all_to_all(to_heads(out_grad), "seq", split_axis=1, concat_axis=0, tiled=True),
    )
    q_rows = moved[0].reshape(own_rows, group_width)
    k_rows = moved[1].reshape(own_rows, group_width)
    v_rows = moved[2].reshape(own_rows, group_width)
    g_rows = moved[3].reshape(own_rows, group_width)
    k_other, v_other = partner((k_rows, v_rows), "seq", 0)

    def in_order(mine, theirs):
        even_rows = jnp.where(is_even, mine, theirs)
        odd_rows = jnp.where(is_even, theirs, mine)
        return jnp.stack([even_rows, odd_rows], axis=1).reshape(2 * mine.shape[0], mine.shape[1])

    key_all = in_order(k_rows, k_other).reshape(length, heads_here, HD)
    value_all = in_order(v_rows, v_other).reshape(length, heads_here, HD)
    query_heads = q_rows.reshape(own_rows, heads_here, HD)
    grad_heads = g_rows.reshape(own_rows, heads_here, HD)
    key_total = jnp.zeros((length, heads_here, HD), jnp.float32)
    value_total = jnp.zeros((length, heads_here, HD), jnp.float32)
    query_parts = []
    for block in range(block_count):
        start = block * block_rows
        stop = start + block_rows
        low = 2 * (start // doc_rows * doc_rows)
        high = 2 * stop
        query_block = query_heads[start:stop]
        grad_block = grad_heads[start:stop]
        key_block = key_all[low:high]
        value_block = value_all[low:high]
        scores = (
            jnp.einsum("qhd,khd->hqk", query_block, key_block, preferred_element_type=jnp.float32)
            * scale
        )
        query_pos = 2 * (start + jnp.arange(block_rows, dtype=jnp.int32)) + parity
        key_pos = low + jnp.arange(high - low, dtype=jnp.int32)
        visible = key_pos[None, :] <= query_pos[:, None]
        scores = jnp.where(visible[None], scores, -jnp.inf)
        top = jnp.max(scores, axis=2, keepdims=True)
        weights = jnp.exp(scores - top)
        probs = weights / jnp.sum(weights, axis=2, keepdims=True)
        probs_low = probs.astype(jnp.bfloat16)
        dprob = jnp.einsum(
            "qhd,khd->hqk", grad_block, value_block, preferred_element_type=jnp.float32
        )
        delta = jnp.sum(probs * dprob, axis=2, keepdims=True)
        dscore = (probs * (dprob - delta) * scale).astype(jnp.bfloat16)
        query_parts.append(
            jnp.einsum(
                "hqk,khd->qhd", dscore, key_block, preferred_element_type=jnp.float32
            ).astype(jnp.bfloat16)
        )
        key_total = key_total.at[low:high].add(
            jnp.einsum("hqk,qhd->khd", dscore, query_block, preferred_element_type=jnp.float32)
        )
        value_total = value_total.at[low:high].add(
            jnp.einsum("hqk,qhd->khd", probs_low, grad_block, preferred_element_type=jnp.float32)
        )
    query_grad = jnp.concatenate(query_parts, axis=0).reshape(own_rows, group_width)

    def by_parity(total):
        paired = total.reshape(own_rows, 2, group_width)
        mine = jnp.where(is_even, paired[:, 0], paired[:, 1])
        theirs = jnp.where(is_even, paired[:, 1], paired[:, 0])
        return (mine.astype(jnp.bfloat16), theirs.astype(jnp.bfloat16))

    key_mine, key_theirs = by_parity(key_total)
    value_mine, value_theirs = by_parity(value_total)
    key_back, value_back = partner((key_theirs, value_theirs), "seq", 0)
    key_grad = (key_mine.astype(jnp.float32) + key_back.astype(jnp.float32)).astype(jnp.bfloat16)
    value_grad = (value_mine.astype(jnp.float32) + value_back.astype(jnp.float32)).astype(
        jnp.bfloat16
    )
    spread = jnp.broadcast_to(
        inputs[0].reshape(half_rows, 1, 2, model_width), (half_rows, groups, 2, model_width)
    ).reshape(half_rows, seq_count, model_width)
    input_rows = lax.all_to_all(spread, "seq", split_axis=1, concat_axis=0, tiled=True).reshape(
        own_rows, model_width
    )
    term = jnp.einsum("td,tc->dc", input_rows, value_grad, preferred_element_type=jnp.float32)
    halves = term.reshape(term.shape[0], 2, term.shape[1] // 2)
    mine = jnp.where(is_even, halves[:, 0], halves[:, 1])
    theirs = jnp.where(is_even, halves[:, 1], halves[:, 0])
    mine, theirs = (mine, theirs)
    received = partner(theirs.astype(jnp.bfloat16), "seq", 0).astype(theirs.dtype)
    weight_grad = lax.psum_scatter(
        (mine + received).astype(jnp.bfloat16), "dp", scatter_dimension=0, tiled=True
    ).astype(jnp.float32)

    def to_tokens(array):
        return array.reshape(seq_count, half_rows, 1, group_width)

    def from_heads(array):
        return (
            array.reshape(half_rows, groups, 2, group_width)
            .transpose(0, 2, 1, 3)
            .reshape(1, tok_rows, width)
        )

    returned = (
        lax.all_to_all(to_tokens(query_grad), "seq", split_axis=0, concat_axis=2, tiled=True),
        lax.all_to_all(to_tokens(key_grad), "seq", split_axis=0, concat_axis=2, tiled=True),
        lax.all_to_all(to_tokens(value_grad), "seq", split_axis=0, concat_axis=2, tiled=True),
    )
    return (from_heads(returned[0]), from_heads(returned[1]), from_heads(returned[2]), weight_grad)


def swap(value, axis, bit):
    return lax.ppermute(value, axis, [(i, i ^ bit) for i in range(lax.axis_size(axis))])


def dot(a, b, dims):
    return lax.dot_general(a, b, (dims, ((), ())), preferred_element_type=jnp.float32)


def probs_by_key(core, queries, keys):
    rows = queries.shape[0]
    scores = dot(keys, queries, ((1,), (1,))) * HD ** (-0.5)
    key_pos = (lax.broadcasted_iota(jnp.int32, (rows, rows), 0) + core * (rows // 2)) & (rows - 1)
    query_pos = (lax.broadcasted_iota(jnp.int32, (rows, rows), 1) + core * (rows // 2)) & (rows - 1)
    scores = jnp.where(key_pos <= query_pos, scores, -jnp.inf)
    weights = jnp.exp(scores - jnp.max(scores, axis=0, keepdims=True))
    return weights * (1.0 / jnp.sum(weights, axis=0, keepdims=True))


def both(mine, theirs):
    return jnp.concatenate([mine[...], theirs[...]], axis=0)


def value_kernel(place, q0, q1, k0, k1, g0, g1, mine, theirs):
    half = q0.shape[0]
    probs = probs_by_key(place[0], both(q0, q1), both(k0, k1))
    grad = dot(probs.astype(jnp.bfloat16), both(g0, g1), ((1,), (0,))).astype(jnp.bfloat16)
    mine[...] = grad[:half]
    theirs[...] = grad[half:]


def value_part(place, head, q, k, g):
    half, width = q[0].shape
    groups = width // (4 * HD)
    taken = pl.BlockSpec((half, HD), lambda i, place: (0, 4 * i + 2 * place[0] + head))
    given = pl.BlockSpec((half, HD), lambda i, place: (0, i))
    out = jax.ShapeDtypeStruct((half, groups * HD), jnp.bfloat16)
    return pl.pallas_call(
        value_kernel,
        grid_spec=pltpu.PrefetchScalarGridSpec(
            num_scalar_prefetch=1, grid=(groups,), in_specs=[taken] * 6, out_specs=[given] * 2
        ),
        out_shape=[out, out],
        name=f"value_part_{head}",
    )(place, *q, *k, *g)


def score_kernel(place, q0, q1, k0, k1, v0, v1, g0, g1, q_mine, q_theirs, k_mine, k_theirs):
    half = q0.shape[0]
    queries, keys = both(q0, q1), both(k0, k1)
    probs = probs_by_key(place[0], queries, keys)
    dprob = dot(both(v0, v1), both(g0, g1), ((1,), (1,)))
    delta = jnp.sum(probs * dprob, axis=0, keepdims=True)
    dscore = (probs * (dprob - delta) * HD ** (-0.5)).astype(jnp.bfloat16)
    key_grad = dot(dscore, queries, ((1,), (0,))).astype(jnp.bfloat16)
    query_grad = dot(dscore, keys, ((0,), (0,))).astype(jnp.bfloat16)
    q_mine[...] = query_grad[:half]
    q_theirs[...] = query_grad[half:]
    k_mine[...] = key_grad[:half]
    k_theirs[...] = key_grad[half:]


def score_part(place, q, k, v, g):
    half, width = q[0].shape
    heads = width // (2 * HD)
    taken = pl.BlockSpec(
        (half, HD), lambda i, place: (0, 4 * (i // 2) + 2 * place[0] + i % 2)
    )
    given = pl.BlockSpec((half, HD), lambda i, place: (0, i))
    out = jax.ShapeDtypeStruct((half, heads * HD), jnp.bfloat16)
    return pl.pallas_call(
        score_kernel,
        grid_spec=pltpu.PrefetchScalarGridSpec(
            num_scalar_prefetch=1, grid=(heads,), in_specs=[taken] * 8, out_specs=[given] * 4
        ),
        out_shape=[out] * 4,
        name="score_part",
    )(place, *q, *k, *v, *g)


def turn_kernel(*refs):
    out = refs[-1]
    rows = refs[0].shape[0]
    for i, piece in enumerate(refs[:-1]):
        out[:, i * rows : (i + 1) * rows] = piece[...].T


def turned(pieces):
    rows, columns = pieces[0].shape
    return pl.pallas_call(
        turn_kernel,
        out_shape=jax.ShapeDtypeStruct((columns, rows * len(pieces)), jnp.bfloat16),
        name="turned",
    )(*pieces)


def term_kernel(place, x_ref, *refs):
    grads, outs, total = refs[:-5], refs[-5:-1], refs[-1]
    values = jnp.concatenate([ref[...] for ref in grads], axis=0)
    total[...] = dot(x_ref[...], values, ((1,), (0,)))
    for apart, out in enumerate(outs):
        start = pl.multiple_of((place[1] ^ apart) * HD, HD)
        out[...] = total[:, pl.ds(start, HD)].astype(out.dtype)


def term_part(place, x_turned, grads):
    rows = x_turned.shape[0]
    vmem = pl.BlockSpec(memory_space=pltpu.VMEM)
    kept = jax.ShapeDtypeStruct((rows, HD), jnp.float32)
    sent = jax.ShapeDtypeStruct((rows, HD), jnp.bfloat16)
    return pl.pallas_call(
        term_kernel,
        in_specs=[pl.BlockSpec(memory_space=pltpu.SMEM)] + [vmem] * (1 + len(grads)),
        out_shape=[kept, sent, sent, sent],
        scratch_shapes=[pltpu.VMEM((rows, grads[0].shape[1]), jnp.float32)],
        name="term_part",
    )(place, x_turned, *grads)


def join_kernel(place, *refs):
    ins, outs = refs[:-3], refs[-3:]
    for mine, first in ((True, 0), (False, 4)):
        core = place[0] if mine else 1 - place[0]
        for out, parts in zip(outs, (ins[first : first + 1], ins[first + 1 : first + 2], ins[first + 2 : first + 4])):
            step = 2 * HD // len(parts)
            for j, part in enumerate(parts):
                for i in range(part.shape[1] // step):
                    start = pl.multiple_of((4 * i + 2 * core) * HD + j * step, HD)
                    out[:, pl.ds(start, step)] = part[:, i * step : (i + 1) * step]


def joined(place, mine, theirs):
    half = mine[0].shape[0]
    width = 2 * mine[0].shape[1]
    vmem = pl.BlockSpec(memory_space=pltpu.VMEM)
    out = jax.ShapeDtypeStruct((half, width), jnp.bfloat16)
    return pl.pallas_call(
        join_kernel,
        in_specs=[pl.BlockSpec(memory_space=pltpu.SMEM)] + [vmem] * 8,
        out_shape=[out] * 3,
        name="joined",
    )(place, *mine, *theirs)


def chip_body(queries, key_vectors, values, out_grad, inputs):
    sample = lax.axis_index("dp")
    spot = lax.axis_index("seq")
    place = jnp.stack([spot % 2, spot // 2]).astype(jnp.int32)
    q, k, g, v = ((a[0], swap(a[0], "seq", 1)) for a in (queries, key_vectors, out_grad, values))

    block = inputs.shape[2] // 4
    x_here = [
        lax.dynamic_slice_in_dim(inputs[0], (sample ^ apart) * block, block, axis=1)
        for apart in range(4)
    ]
    x_mine = [x_here[0]] + [swap(x_here[apart], "dp", apart) for apart in (1, 2, 3)]
    x_pieces = []
    for piece in x_mine:
        x_pieces += [piece, swap(piece, "seq", 1)]
    x_turned = turned(x_pieces)

    value_mine, value_theirs, own, received = [], [], [], []
    for head in range(2):
        a, b = value_part(place, head, q, k, g)
        value_mine.append(a)
        value_theirs.append(b)
    for head in range(2):
        a, b = value_mine[head], value_theirs[head]
        a_y, b_x = swap(a, "dp", 2), swap(b, "dp", 1)
        b_y, a_x = swap(b, "dp", 2), swap(a, "dp", 1)
        a_xy, b_xy = swap(a_y, "dp", 1), swap(b_x, "dp", 2)
        term = term_part(place, x_turned, [a, b, a_x, b_x, a_y, b_y, a_xy, b_xy])
        own.append(term[0])
        received.append([swap(term[apart], "seq", 2 * apart) for apart in (1, 2, 3)])
    weight_grad = jnp.concatenate(
        [
            mine + sum(part.astype(jnp.float32) for part in parts)
            for mine, parts in zip(own, received)
        ],
        axis=1,
    )

    q_mine, q_theirs, k_mine, k_theirs = score_part(place, q, k, v, g)
    back = [swap(a, "seq", 1) for a in (q_theirs, k_theirs, *value_theirs)]
    query_grad, key_grad, value_grad = joined(place, [q_mine, k_mine, *value_mine], back)
    return query_grad[None], key_grad[None], value_grad[None], weight_grad


def solution(mesh):
    on_chip = mesh.shape["dp"] == 4 and mesh.shape["seq"] == 8
    return jax.shard_map(
        chip_body if on_chip else body,
        mesh=mesh,
        in_specs=(
            P("dp", "seq", None),
            P("dp", "seq", None),
            P("dp", "seq", None),
            P("dp", "seq", None),
            P("dp", "seq", None),
        ),
        out_specs=(
            P("dp", "seq", None),
            P("dp", "seq", None),
            P("dp", "seq", None),
            P("dp", "seq"),
        ),
        check_vma=False,
    )
```

```python
import jax
import jax.numpy as jnp
from jax import lax
from jax.experimental import pallas as pl
from jax.experimental.pallas import tpu as pltpu
from jax.sharding import PartitionSpec as P

HD = 128


def partner(value, axis, apart):
    return lax.ppermute(value, axis, [(i, i ^ 1 << apart) for i in range(lax.axis_size(axis))])


def body(queries, key_vectors, values, out_grad, inputs):
    seq_count = lax.axis_size("seq")
    groups = seq_count // 2
    parity = lax.axis_index("seq") % 2
    is_even = parity == 0
    tok_rows = queries.shape[1]
    half_rows = tok_rows // 2
    width = queries.shape[2]
    group_width = 2 * width // seq_count
    heads_here = group_width // HD
    model_width = inputs.shape[2]
    own_rows = seq_count * half_rows
    length = 2 * own_rows
    doc_rows = own_rows // 4
    block_rows = min(doc_rows, max(256, length // 16))
    block_count = own_rows // block_rows
    scale = HD ** (-0.5)

    def to_heads(array):
        return (
            array[0]
            .reshape(half_rows, 2, groups, group_width)
            .transpose(0, 2, 1, 3)
            .reshape(half_rows, seq_count, group_width)
        )

    moved = (
        lax.all_to_all(to_heads(queries), "seq", split_axis=1, concat_axis=0, tiled=True),
        lax.all_to_all(to_heads(key_vectors), "seq", split_axis=1, concat_axis=0, tiled=True),
        lax.all_to_all(to_heads(values), "seq", split_axis=1, concat_axis=0, tiled=True),
        lax.all_to_all(to_heads(out_grad), "seq", split_axis=1, concat_axis=0, tiled=True),
    )
    q_rows = moved[0].reshape(own_rows, group_width)
    k_rows = moved[1].reshape(own_rows, group_width)
    v_rows = moved[2].reshape(own_rows, group_width)
    g_rows = moved[3].reshape(own_rows, group_width)
    k_other, v_other = partner((k_rows, v_rows), "seq", 0)

    def in_order(mine, theirs):
        even_rows = jnp.where(is_even, mine, theirs)
        odd_rows = jnp.where(is_even, theirs, mine)
        return jnp.stack([even_rows, odd_rows], axis=1).reshape(2 * mine.shape[0], mine.shape[1])

    key_all = in_order(k_rows, k_other).reshape(length, heads_here, HD)
    value_all = in_order(v_rows, v_other).reshape(length, heads_here, HD)
    query_heads = q_rows.reshape(own_rows, heads_here, HD)
    grad_heads = g_rows.reshape(own_rows, heads_here, HD)
    key_total = jnp.zeros((length, heads_here, HD), jnp.float32)
    value_total = jnp.zeros((length, heads_here, HD), jnp.float32)
    query_parts = []
    for block in range(block_count):
        start = block * block_rows
        stop = start + block_rows
        low = 2 * (start // doc_rows * doc_rows)
        high = 2 * stop
        query_block = query_heads[start:stop]
        grad_block = grad_heads[start:stop]
        key_block = key_all[low:high]
        value_block = value_all[low:high]
        scores = (
            jnp.einsum("qhd,khd->hqk", query_block, key_block, preferred_element_type=jnp.float32)
            * scale
        )
        query_pos = 2 * (start + jnp.arange(block_rows, dtype=jnp.int32)) + parity
        key_pos = low + jnp.arange(high - low, dtype=jnp.int32)
        visible = key_pos[None, :] <= query_pos[:, None]
        scores = jnp.where(visible[None], scores, -jnp.inf)
        top = jnp.max(scores, axis=2, keepdims=True)
        weights = jnp.exp(scores - top)
        probs = weights / jnp.sum(weights, axis=2, keepdims=True)
        probs_low = probs.astype(jnp.bfloat16)
        dprob = jnp.einsum(
            "qhd,khd->hqk", grad_block, value_block, preferred_element_type=jnp.float32
        )
        delta = jnp.sum(probs * dprob, axis=2, keepdims=True)
        dscore = (probs * (dprob - delta) * scale).astype(jnp.bfloat16)
        query_parts.append(
            jnp.einsum(
                "hqk,khd->qhd", dscore, key_block, preferred_element_type=jnp.float32
            ).astype(jnp.bfloat16)
        )
        key_total = key_total.at[low:high].add(
            jnp.einsum("hqk,qhd->khd", dscore, query_block, preferred_element_type=jnp.float32)
        )
        value_total = value_total.at[low:high].add(
            jnp.einsum("hqk,qhd->khd", probs_low, grad_block, preferred_element_type=jnp.float32)
        )
    query_grad = jnp.concatenate(query_parts, axis=0).reshape(own_rows, group_width)

    def by_parity(total):
        paired = total.reshape(own_rows, 2, group_width)
        mine = jnp.where(is_even, paired[:, 0], paired[:, 1])
        theirs = jnp.where(is_even, paired[:, 1], paired[:, 0])
        return (mine.astype(jnp.bfloat16), theirs.astype(jnp.bfloat16))

    key_mine, key_theirs = by_parity(key_total)
    value_mine, value_theirs = by_parity(value_total)
    key_back, value_back = partner((key_theirs, value_theirs), "seq", 0)
    key_grad = (key_mine.astype(jnp.float32) + key_back.astype(jnp.float32)).astype(jnp.bfloat16)
    value_grad = (value_mine.astype(jnp.float32) + value_back.astype(jnp.float32)).astype(
        jnp.bfloat16
    )
    spread = jnp.broadcast_to(
        inputs[0].reshape(half_rows, 1, 2, model_width), (half_rows, groups, 2, model_width)
    ).reshape(half_rows, seq_count, model_width)
    input_rows = lax.all_to_all(spread, "seq", split_axis=1, concat_axis=0, tiled=True).reshape(
        own_rows, model_width
    )
    term = jnp.einsum("td,tc->dc", input_rows, value_grad, preferred_element_type=jnp.float32)
    halves = term.reshape(term.shape[0], 2, term.shape[1] // 2)
    mine = jnp.where(is_even, halves[:, 0], halves[:, 1])
    theirs = jnp.where(is_even, halves[:, 1], halves[:, 0])
    mine, theirs = (mine, theirs)
    received = partner(theirs.astype(jnp.bfloat16), "seq", 0).astype(theirs.dtype)
    weight_grad = lax.psum_scatter(
        (mine + received).astype(jnp.bfloat16), "dp", scatter_dimension=0, tiled=True
    ).astype(jnp.float32)

    def to_tokens(array):
        return array.reshape(seq_count, half_rows, 1, group_width)

    def from_heads(array):
        return (
            array.reshape(half_rows, groups, 2, group_width)
            .transpose(0, 2, 1, 3)
            .reshape(1, tok_rows, width)
        )

    returned = (
        lax.all_to_all(to_tokens(query_grad), "seq", split_axis=0, concat_axis=2, tiled=True),
        lax.all_to_all(to_tokens(key_grad), "seq", split_axis=0, concat_axis=2, tiled=True),
        lax.all_to_all(to_tokens(value_grad), "seq", split_axis=0, concat_axis=2, tiled=True),
    )
    return (from_heads(returned[0]), from_heads(returned[1]), from_heads(returned[2]), weight_grad)


def swap(value, axis, bit):
    return lax.ppermute(value, axis, [(i, i ^ bit) for i in range(lax.axis_size(axis))])


def dot(a, b, dims):
    return lax.dot_general(a, b, (dims, ((), ())), preferred_element_type=jnp.float32)


def local_call(kernel, name, outs, scratch=()):
    in_vmem = pl.BlockSpec(memory_space=pltpu.VMEM)

    def call(*operands):
        return pl.pallas_call(
            kernel,
            in_specs=[in_vmem] * len(operands),
            out_specs=[in_vmem] * len(outs),
            out_shape=outs,
            scratch_shapes=scratch,
            compiler_params=pltpu.CompilerParams(vmem_limit_bytes=16 << 20),
            name=name,
        )(*(pltpu.with_memory_space_constraint(a, pltpu.VMEM) for a in operands))

    return call


def columns(start):
    return pl.ds(pl.multiple_of(start * HD, HD), HD)


def both(mine, theirs, where):
    return jnp.concatenate([mine[:, where], theirs[:, where]], axis=0)


def probs_by_key(core, queries, keys):
    rows = queries.shape[0]
    scores = dot(keys, queries, ((1,), (1,))) * HD ** (-0.5)
    key_pos = (lax.broadcasted_iota(jnp.int32, (rows, rows), 0) + core * (rows // 2)) & (rows - 1)
    query_pos = (lax.broadcasted_iota(jnp.int32, (rows, rows), 1) + core * (rows // 2)) & (rows - 1)
    scores = jnp.where(key_pos <= query_pos, scores, -jnp.inf)
    weights = jnp.exp(scores - jnp.max(scores, axis=0, keepdims=True))
    return weights * (1.0 / jnp.sum(weights, axis=0, keepdims=True))


def value_part(head, q, k, g):
    half, width = q[0].shape
    groups = width // (4 * HD)

    def kernel(q0, q1, k0, k1, g0, g1, out):
        core = lax.axis_index("seq") % 2
        for group in range(groups):
            where = columns(4 * group + 2 * core + head)
            probs = probs_by_key(core, both(q0, q1, where), both(k0, k1, where))
            grad = dot(probs.astype(jnp.bfloat16), both(g0, g1, where), ((1,), (0,)))
            out[:, group * HD : (group + 1) * HD] = grad.astype(jnp.bfloat16)

    out = pltpu.VMEM((2 * half, groups * HD), jnp.bfloat16)
    return local_call(kernel, f"value_part_{head}", [out])(*q, *k, *g)[0]


def score_part(q, k, v, g):
    half, width = q[0].shape
    heads = width // (2 * HD)

    def kernel(q0, q1, k0, k1, v0, v1, g0, g1, q_mine, q_theirs, k_mine, k_theirs):
        core = lax.axis_index("seq") % 2
        for head in range(heads):
            where = columns(4 * (head // 2) + 2 * core + head % 2)
            queries, keys = both(q0, q1, where), both(k0, k1, where)
            probs = probs_by_key(core, queries, keys)
            dprob = dot(both(v0, v1, where), both(g0, g1, where), ((1,), (1,)))
            delta = jnp.sum(probs * dprob, axis=0, keepdims=True)
            dscore = (probs * (dprob - delta) * HD ** (-0.5)).astype(jnp.bfloat16)
            key_grad = dot(dscore, queries, ((1,), (0,))).astype(jnp.bfloat16)
            query_grad = dot(dscore, keys, ((0,), (0,))).astype(jnp.bfloat16)
            there = slice(head * HD, (head + 1) * HD)
            q_mine[:, there] = query_grad[:half]
            q_theirs[:, there] = query_grad[half:]
            k_mine[:, there] = key_grad[:half]
            k_theirs[:, there] = key_grad[half:]

    out = pltpu.VMEM((half, heads * HD), jnp.bfloat16)
    return local_call(kernel, "score_part", [out] * 4)(*q, *k, *v, *g)


def turned(pieces):
    rows, width = pieces[0].shape

    def kernel(*refs):
        for i, piece in enumerate(refs[:-1]):
            refs[-1][:, i * rows : (i + 1) * rows] = piece[...].T

    out = pltpu.VMEM((width, rows * len(pieces)), jnp.bfloat16)
    return local_call(kernel, "turned", [out])(*pieces)[0]


def term_part(x_turned, grads):
    rows = x_turned.shape[0]

    def kernel(x_ref, *refs):
        grads, outs, total = refs[:-5], refs[-5:-1], refs[-1]
        chip = lax.axis_index("seq") // 2
        values = jnp.concatenate([ref[...] for ref in grads], axis=0)
        total[...] = dot(x_ref[...], values, ((1,), (0,)))
        for apart, out in enumerate(outs):
            out[...] = total[:, columns(chip ^ apart)].astype(out.dtype)

    kept = pltpu.VMEM((rows, HD), jnp.float32)
    sent = pltpu.VMEM((rows, HD), jnp.bfloat16)
    scratch = [pltpu.VMEM((rows, grads[0].shape[1]), jnp.float32)]
    return local_call(kernel, "term_part", [kept, sent, sent, sent], scratch)(x_turned, *grads)


def joined(mine, theirs):
    half = mine[0].shape[0]
    width = 2 * mine[0].shape[1]

    def kernel(*refs):
        outs = refs[-3:]
        core = lax.axis_index("seq") % 2
        for ins, owner in ((refs[:4], core), (refs[4:8], 1 - core)):
            for i in range(width // (4 * HD)):
                for j in range(2):
                    where = columns(4 * i + 2 * owner + j)
                    here = slice((2 * i + j) * HD, (2 * i + j + 1) * HD)
                    outs[0][:, where] = ins[0][:, here]
                    outs[1][:, where] = ins[1][:, here]
                    outs[2][:, where] = ins[2 + j][:, i * HD : (i + 1) * HD]

    out = jax.ShapeDtypeStruct((half, width), jnp.bfloat16)
    return local_call(kernel, "joined", [out] * 3)(*mine, *theirs)


def chip_body(queries, key_vectors, values, out_grad, inputs):
    sample = lax.axis_index("dp")
    q, k, g, v = ((a[0], swap(a[0], "seq", 1)) for a in (queries, key_vectors, out_grad, values))

    block = inputs.shape[2] // 4
    x_here = [
        lax.dynamic_slice_in_dim(inputs[0], (sample ^ apart) * block, block, axis=1)
        for apart in range(4)
    ]
    x_mine = [x_here[0]] + [swap(x_here[apart], "dp", apart) for apart in (1, 2, 3)]

    grads = [value_part(head, q, k, g) for head in range(2)]
    *x_mine, grads[1] = lax.optimization_barrier((*x_mine, grads[1]))
    x_pieces = [a for piece in x_mine for a in (piece, swap(piece, "seq", 1))]
    x_turned = turned(x_pieces)

    half = queries.shape[1]
    own, received = [], []
    for grad in grads:
        by_x, by_y = swap(grad, "dp", 1), swap(grad, "dp", 2)
        first, second = swap(by_y[:half], "dp", 1), swap(by_x[half:], "dp", 2)
        term = term_part(x_turned, [grad, by_x, by_y, first, second])
        own.append(term[0])
        received.append([swap(term[apart], "seq", 2 * apart) for apart in (1, 2, 3)])
    weight_grad = jnp.concatenate(
        [
            mine + sum(part.astype(jnp.float32) for part in parts)
            for mine, parts in zip(own, received)
        ],
        axis=1,
    )

    q_mine, q_theirs, k_mine, k_theirs = score_part(q, k, v, g)
    back = [swap(a, "seq", 1) for a in (q_theirs, k_theirs, grads[0][half:], grads[1][half:])]
    query_grad, key_grad, value_grad = joined(
        [q_mine, k_mine, grads[0][:half], grads[1][:half]], back
    )
    return query_grad[None], key_grad[None], value_grad[None], weight_grad


def solution(mesh):
    on_chip = mesh.shape["dp"] == 4 and mesh.shape["seq"] == 8
    return jax.shard_map(
        chip_body if on_chip else body,
        mesh=mesh,
        in_specs=(
            P("dp", "seq", None),
            P("dp", "seq", None),
            P("dp", "seq", None),
            P("dp", "seq", None),
            P("dp", "seq", None),
        ),
        out_specs=(
            P("dp", "seq", None),
            P("dp", "seq", None),
            P("dp", "seq", None),
            P("dp", "seq"),
        ),
        check_vma=False,
    )
```

```python
import jax
import jax.numpy as jnp
from jax import lax
from jax.experimental import pallas as pl
from jax.experimental.pallas import tpu as pltpu
from jax.sharding import PartitionSpec as P

HD = 128


def partner(value, axis, apart):
    return lax.ppermute(value, axis, [(i, i ^ 1 << apart) for i in range(lax.axis_size(axis))])


def body(queries, key_vectors, values, out_grad, inputs):
    seq_count = lax.axis_size("seq")
    groups = seq_count // 2
    parity = lax.axis_index("seq") % 2
    is_even = parity == 0
    tok_rows = queries.shape[1]
    half_rows = tok_rows // 2
    width = queries.shape[2]
    group_width = 2 * width // seq_count
    heads_here = group_width // HD
    model_width = inputs.shape[2]
    own_rows = seq_count * half_rows
    length = 2 * own_rows
    doc_rows = own_rows // 4
    block_rows = min(doc_rows, max(256, length // 16))
    block_count = own_rows // block_rows
    scale = HD ** (-0.5)

    def to_heads(array):
        return (
            array[0]
            .reshape(half_rows, 2, groups, group_width)
            .transpose(0, 2, 1, 3)
            .reshape(half_rows, seq_count, group_width)
        )

    moved = (
        lax.all_to_all(to_heads(queries), "seq", split_axis=1, concat_axis=0, tiled=True),
        lax.all_to_all(to_heads(key_vectors), "seq", split_axis=1, concat_axis=0, tiled=True),
        lax.all_to_all(to_heads(values), "seq", split_axis=1, concat_axis=0, tiled=True),
        lax.all_to_all(to_heads(out_grad), "seq", split_axis=1, concat_axis=0, tiled=True),
    )
    q_rows = moved[0].reshape(own_rows, group_width)
    k_rows = moved[1].reshape(own_rows, group_width)
    v_rows = moved[2].reshape(own_rows, group_width)
    g_rows = moved[3].reshape(own_rows, group_width)
    k_other, v_other = partner((k_rows, v_rows), "seq", 0)

    def in_order(mine, theirs):
        even_rows = jnp.where(is_even, mine, theirs)
        odd_rows = jnp.where(is_even, theirs, mine)
        return jnp.stack([even_rows, odd_rows], axis=1).reshape(2 * mine.shape[0], mine.shape[1])

    key_all = in_order(k_rows, k_other).reshape(length, heads_here, HD)
    value_all = in_order(v_rows, v_other).reshape(length, heads_here, HD)
    query_heads = q_rows.reshape(own_rows, heads_here, HD)
    grad_heads = g_rows.reshape(own_rows, heads_here, HD)
    key_total = jnp.zeros((length, heads_here, HD), jnp.float32)
    value_total = jnp.zeros((length, heads_here, HD), jnp.float32)
    query_parts = []
    for block in range(block_count):
        start = block * block_rows
        stop = start + block_rows
        low = 2 * (start // doc_rows * doc_rows)
        high = 2 * stop
        query_block = query_heads[start:stop]
        grad_block = grad_heads[start:stop]
        key_block = key_all[low:high]
        value_block = value_all[low:high]
        scores = (
            jnp.einsum("qhd,khd->hqk", query_block, key_block, preferred_element_type=jnp.float32)
            * scale
        )
        query_pos = 2 * (start + jnp.arange(block_rows, dtype=jnp.int32)) + parity
        key_pos = low + jnp.arange(high - low, dtype=jnp.int32)
        visible = key_pos[None, :] <= query_pos[:, None]
        scores = jnp.where(visible[None], scores, -jnp.inf)
        top = jnp.max(scores, axis=2, keepdims=True)
        weights = jnp.exp(scores - top)
        probs = weights / jnp.sum(weights, axis=2, keepdims=True)
        probs_low = probs.astype(jnp.bfloat16)
        dprob = jnp.einsum(
            "qhd,khd->hqk", grad_block, value_block, preferred_element_type=jnp.float32
        )
        delta = jnp.sum(probs * dprob, axis=2, keepdims=True)
        dscore = (probs * (dprob - delta) * scale).astype(jnp.bfloat16)
        query_parts.append(
            jnp.einsum(
                "hqk,khd->qhd", dscore, key_block, preferred_element_type=jnp.float32
            ).astype(jnp.bfloat16)
        )
        key_total = key_total.at[low:high].add(
            jnp.einsum("hqk,qhd->khd", dscore, query_block, preferred_element_type=jnp.float32)
        )
        value_total = value_total.at[low:high].add(
            jnp.einsum("hqk,qhd->khd", probs_low, grad_block, preferred_element_type=jnp.float32)
        )
    query_grad = jnp.concatenate(query_parts, axis=0).reshape(own_rows, group_width)

    def by_parity(total):
        paired = total.reshape(own_rows, 2, group_width)
        mine = jnp.where(is_even, paired[:, 0], paired[:, 1])
        theirs = jnp.where(is_even, paired[:, 1], paired[:, 0])
        return (mine.astype(jnp.bfloat16), theirs.astype(jnp.bfloat16))

    key_mine, key_theirs = by_parity(key_total)
    value_mine, value_theirs = by_parity(value_total)
    key_back, value_back = partner((key_theirs, value_theirs), "seq", 0)
    key_grad = (key_mine.astype(jnp.float32) + key_back.astype(jnp.float32)).astype(jnp.bfloat16)
    value_grad = (value_mine.astype(jnp.float32) + value_back.astype(jnp.float32)).astype(
        jnp.bfloat16
    )
    spread = jnp.broadcast_to(
        inputs[0].reshape(half_rows, 1, 2, model_width), (half_rows, groups, 2, model_width)
    ).reshape(half_rows, seq_count, model_width)
    input_rows = lax.all_to_all(spread, "seq", split_axis=1, concat_axis=0, tiled=True).reshape(
        own_rows, model_width
    )
    term = jnp.einsum("td,tc->dc", input_rows, value_grad, preferred_element_type=jnp.float32)
    halves = term.reshape(term.shape[0], 2, term.shape[1] // 2)
    mine = jnp.where(is_even, halves[:, 0], halves[:, 1])
    theirs = jnp.where(is_even, halves[:, 1], halves[:, 0])
    mine, theirs = (mine, theirs)
    received = partner(theirs.astype(jnp.bfloat16), "seq", 0).astype(theirs.dtype)
    weight_grad = lax.psum_scatter(
        (mine + received).astype(jnp.bfloat16), "dp", scatter_dimension=0, tiled=True
    ).astype(jnp.float32)

    def to_tokens(array):
        return array.reshape(seq_count, half_rows, 1, group_width)

    def from_heads(array):
        return (
            array.reshape(half_rows, groups, 2, group_width)
            .transpose(0, 2, 1, 3)
            .reshape(1, tok_rows, width)
        )

    returned = (
        lax.all_to_all(to_tokens(query_grad), "seq", split_axis=0, concat_axis=2, tiled=True),
        lax.all_to_all(to_tokens(key_grad), "seq", split_axis=0, concat_axis=2, tiled=True),
        lax.all_to_all(to_tokens(value_grad), "seq", split_axis=0, concat_axis=2, tiled=True),
    )
    return (from_heads(returned[0]), from_heads(returned[1]), from_heads(returned[2]), weight_grad)


def swap(value, axis, bit):
    return lax.ppermute(value, axis, [(i, i ^ bit) for i in range(lax.axis_size(axis))])


def dot(a, b, dims):
    return lax.dot_general(a, b, (dims, ((), ())), preferred_element_type=jnp.float32)


def local_call(kernel, name, outs, scratch=()):
    in_vmem = pl.BlockSpec(memory_space=pltpu.VMEM)

    def call(*operands):
        return pl.pallas_call(
            kernel,
            in_specs=[in_vmem] * len(operands),
            out_specs=[in_vmem] * len(outs),
            out_shape=outs,
            scratch_shapes=scratch,
            compiler_params=pltpu.CompilerParams(vmem_limit_bytes=16 << 20),
            name=name,
        )(*(pltpu.with_memory_space_constraint(a, pltpu.VMEM) for a in operands))

    return call


def columns(start):
    return pl.ds(pl.multiple_of(start * HD, HD), HD)


def both(mine, theirs, group, core, head):
    packed, spread = columns(2 * group + head), columns(4 * group + 2 * core + head)
    return jnp.concatenate([mine[:, packed], theirs[:, spread]], axis=0)


def packed_inputs(arrays, inputs):
    half, width = arrays[0].shape
    block = inputs.shape[1] // 4
    count = len(arrays)
    groups = width // (4 * HD)

    def kernel(*refs):
        core, sample = lax.axis_index("seq") % 2, lax.axis_index("dp")
        outs, sems = refs[count + 1 : -1], refs[-1]
        copies = []
        for apart, out in enumerate(outs[count:]):
            start = pl.multiple_of((sample ^ apart) * block, block)
            copies.append((refs[count].at[:, pl.ds(start, block)], out))
        for source, out in zip(refs[:count], outs):
            for group in range(groups):
                start = pl.multiple_of((4 * group + 2 * core) * HD, 2 * HD)
                here = slice(2 * group * HD, 2 * (group + 1) * HD)
                copies.append((source.at[:, pl.ds(start, 2 * HD)], out.at[:, here]))
        copies = [pltpu.make_async_copy(a, b, sems.at[i]) for i, (a, b) in enumerate(copies)]
        for copy in copies:
            copy.start()
        for copy in copies:
            copy.wait()

    return pl.pallas_call(
        kernel,
        in_specs=[pl.BlockSpec(memory_space=pl.ANY)] * (count + 1),
        out_specs=[pl.BlockSpec(memory_space=pltpu.VMEM)] * (count + 4),
        out_shape=[pltpu.VMEM((half, width // 2), jnp.bfloat16)] * count
        + [pltpu.VMEM((half, block), jnp.bfloat16)] * 4,
        scratch_shapes=[pltpu.SemaphoreType.DMA((4 + count * groups,))],
        compiler_params=pltpu.CompilerParams(vmem_limit_bytes=16 << 20),
        name="packed_inputs",
    )(*(pltpu.with_memory_space_constraint(a, pltpu.HBM) for a in (*arrays, inputs)))


def probs_by_key(core, queries, keys):
    rows = queries.shape[0]
    scores = dot(keys, queries, ((1,), (1,))) * HD ** (-0.5)
    key_pos = (lax.broadcasted_iota(jnp.int32, (rows, rows), 0) + core * (rows // 2)) & (rows - 1)
    query_pos = (lax.broadcasted_iota(jnp.int32, (rows, rows), 1) + core * (rows // 2)) & (rows - 1)
    scores = jnp.where(key_pos <= query_pos, scores, -jnp.inf)
    weights = jnp.exp(scores - jnp.max(scores, axis=0, keepdims=True))
    return weights * (1.0 / jnp.sum(weights, axis=0, keepdims=True))


def value_part(q, k, g):
    half, width = q[1].shape
    order = (0, 2, 1, 3)

    def kernel(q0, q1, k0, k1, g0, g1, kept, given):
        core, chip = lax.axis_index("seq") % 2, lax.axis_index("seq") // 2
        for at, apart in enumerate(order):
            for head in range(2):
                where = chip ^ apart, core, head
                probs = probs_by_key(core, both(q0, q1, *where), both(k0, k1, *where))
                grad = dot(probs.astype(jnp.bfloat16), both(g0, g1, *where), ((1,), (0,)))
                here = (2 * head + at % 2) * HD
                (kept, given)[at // 2][:, here : here + HD] = grad.astype(jnp.bfloat16)

    out = pltpu.VMEM((2 * half, width // 4), jnp.bfloat16)
    return local_call(kernel, "value_part", [out] * 2)(*q, *k, *g)


def score_part(q, k, v, g):
    half, width = q[1].shape
    heads = width // (2 * HD)

    def kernel(q0, q1, k0, k1, v0, v1, g0, g1, q_mine, q_theirs, k_mine, k_theirs):
        core = lax.axis_index("seq") % 2
        for head in range(heads):
            where = head // 2, core, head % 2
            queries, keys = both(q0, q1, *where), both(k0, k1, *where)
            probs = probs_by_key(core, queries, keys)
            dprob = dot(both(v0, v1, *where), both(g0, g1, *where), ((1,), (1,)))
            delta = jnp.sum(probs * dprob, axis=0, keepdims=True)
            dscore = (probs * (dprob - delta) * HD ** (-0.5)).astype(jnp.bfloat16)
            key_grad = dot(dscore, queries, ((1,), (0,))).astype(jnp.bfloat16)
            query_grad = dot(dscore, keys, ((0,), (0,))).astype(jnp.bfloat16)
            there = slice(head * HD, (head + 1) * HD)
            q_mine[:, there] = query_grad[:half]
            q_theirs[:, there] = query_grad[half:]
            k_mine[:, there] = key_grad[:half]
            k_theirs[:, there] = key_grad[half:]

    out = pltpu.VMEM((half, heads * HD), jnp.bfloat16)
    return local_call(kernel, "score_part", [out] * 4)(*q, *k, *v, *g)


def turned(pieces):
    rows, width = pieces[0].shape

    def kernel(*refs):
        for i, piece in enumerate(refs[:-1]):
            refs[-1][:, i * rows : (i + 1) * rows] = piece[...].T

    out = pltpu.VMEM((width, rows * len(pieces)), jnp.bfloat16)
    return local_call(kernel, "turned", [out])(*pieces)[0]


def term_part(turned_inputs, near, far):
    rows = turned_inputs[0].shape[0]
    width = near[0].shape[1] // 2
    half = near[0].shape[0] // 2
    count = len(near)

    def kernel(*refs):
        outs = refs[-2:]
        total = None
        for i, x_ref in enumerate(refs[:4]):
            values = refs[4 + i // 2 * count : 4 + (i // 2 + 1) * count]
            here = slice(i % 2 * half, (i % 2 + 1) * half)
            part = jnp.concatenate([ref[here, :] for ref in values], axis=0)
            product = dot(x_ref[...], part, ((1,), (0,)))
            total = product if total is None else total + product
        for i, out in enumerate(outs):
            out[...] = total[:, i * width : (i + 1) * width].astype(out.dtype)

    outs = [pltpu.VMEM((rows, width), kind) for kind in (jnp.float32, jnp.bfloat16)]
    return local_call(kernel, "term_part", outs)(*turned_inputs, *near, *far)


def joined(mine, theirs):
    half = mine[0].shape[0]
    width = 2 * mine[0].shape[1]

    def kernel(*refs):
        outs = refs[-3:]
        core, chip = lax.axis_index("seq") % 2, lax.axis_index("seq") // 2
        for ins, owner in ((refs[:4], core), (refs[4:8], 1 - core)):
            for i in range(width // (4 * HD)):
                for j in range(2):
                    where = columns(4 * i + 2 * owner + j)
                    here = slice((2 * i + j) * HD, (2 * i + j + 1) * HD)
                    outs[0][:, where] = ins[0][:, here]
                    outs[1][:, where] = ins[1][:, here]
                    where = columns(4 * (chip ^ i) + 2 * owner + j)
                    here = slice((2 * j + i // 2) * HD, (2 * j + i // 2 + 1) * HD)
                    outs[2][:, where] = ins[2 + i % 2][:, here]

    out = jax.ShapeDtypeStruct((half, width), jnp.bfloat16)
    return local_call(kernel, "joined", [out] * 3)(*mine, *theirs)


def after(values, *earlier):
    return list(lax.optimization_barrier((*values, *earlier))[: len(values)])


def chip_body(queries, key_vectors, values, out_grad, inputs):
    half = queries.shape[1]
    arrays = [a[0] for a in (queries, key_vectors, out_grad, values)]
    *own, x_here, x_1, x_2, x_3 = packed_inputs(arrays, inputs[0])
    q, k, g, v = ((mine, swap(a, "seq", 1)) for mine, a in zip(own, arrays))
    x_mine = [x_here, swap(x_1, "dp", 1), swap(x_2, "dp", 2), swap(x_3, "dp", 3)]

    kept, given = value_part(q, k, g)
    q_mine, q_theirs, k_mine, k_theirs = score_part(q, k, v, g)
    back = [swap(a, "seq", 1) for a in (q_theirs, k_theirs, kept[half:], given[half:])]
    query_grad, key_grad, value_grad = joined([q_mine, k_mine, kept[:half], given[:half]], back)
    got = swap(given, "seq", 2)
    sides = []
    for head in range(2):
        here = slice(2 * head * HD, 2 * (head + 1) * HD)
        paired = jnp.concatenate([kept[:, here], got[:, here]], axis=0)
        by_x, by_y = after([swap(paired, "dp", 1), swap(paired, "dp", 2)])
        first, second = after([swap(by_y[: 2 * half], "dp", 1), swap(by_x[2 * half :], "dp", 2)])
        near = [paired[: 2 * half], by_x[: 2 * half], by_y[: 2 * half], first]
        far = [paired[2 * half :], by_x[2 * half :], by_y[2 * half :], second]
        sides.append((near, far))

    x_mine = after(x_mine, got, q_theirs)
    x_own = turned(x_mine)
    x_next = swap([x_own][0], "seq", 2)
    x_turned = [x_own, swap(x_own, "seq", 1), x_next, swap(after([x_next], query_grad)[0], "seq", 1)]

    blocks = []
    for near, far in sides:
        mine, sent = term_part(x_turned, near, far)
        blocks.append(mine + swap(sent, "seq", 4).astype(jnp.float32))
    weight_grad = jnp.concatenate(blocks, axis=1)

    return query_grad[None], key_grad[None], value_grad[None], weight_grad


def solution(mesh):
    on_chip = mesh.shape["dp"] == 4 and mesh.shape["seq"] == 8
    return jax.shard_map(
        chip_body if on_chip else body,
        mesh=mesh,
        in_specs=(
            P("dp", "seq", None),
            P("dp", "seq", None),
            P("dp", "seq", None),
            P("dp", "seq", None),
            P("dp", "seq", None),
        ),
        out_specs=(
            P("dp", "seq", None),
            P("dp", "seq", None),
            P("dp", "seq", None),
            P("dp", "seq"),
        ),
        check_vma=False,
    )
```

```python
import jax
import jax.numpy as jnp
from jax import lax
from jax.experimental import pallas as pl
from jax.experimental.pallas import tpu as pltpu
from jax.sharding import PartitionSpec as P

HD = 128


def partner(value, axis, apart):
    return lax.ppermute(value, axis, [(i, i ^ 1 << apart) for i in range(lax.axis_size(axis))])


def body(queries, key_vectors, values, out_grad, inputs):
    seq_count = lax.axis_size("seq")
    groups = seq_count // 2
    parity = lax.axis_index("seq") % 2
    is_even = parity == 0
    tok_rows = queries.shape[1]
    half_rows = tok_rows // 2
    width = queries.shape[2]
    group_width = 2 * width // seq_count
    heads_here = group_width // HD
    model_width = inputs.shape[2]
    own_rows = seq_count * half_rows
    length = 2 * own_rows
    doc_rows = own_rows // 4
    block_rows = min(doc_rows, max(256, length // 16))
    block_count = own_rows // block_rows
    scale = HD ** (-0.5)

    def to_heads(array):
        return (
            array[0]
            .reshape(half_rows, 2, groups, group_width)
            .transpose(0, 2, 1, 3)
            .reshape(half_rows, seq_count, group_width)
        )

    moved = (
        lax.all_to_all(to_heads(queries), "seq", split_axis=1, concat_axis=0, tiled=True),
        lax.all_to_all(to_heads(key_vectors), "seq", split_axis=1, concat_axis=0, tiled=True),
        lax.all_to_all(to_heads(values), "seq", split_axis=1, concat_axis=0, tiled=True),
        lax.all_to_all(to_heads(out_grad), "seq", split_axis=1, concat_axis=0, tiled=True),
    )
    q_rows = moved[0].reshape(own_rows, group_width)
    k_rows = moved[1].reshape(own_rows, group_width)
    v_rows = moved[2].reshape(own_rows, group_width)
    g_rows = moved[3].reshape(own_rows, group_width)
    k_other, v_other = partner((k_rows, v_rows), "seq", 0)

    def in_order(mine, theirs):
        even_rows = jnp.where(is_even, mine, theirs)
        odd_rows = jnp.where(is_even, theirs, mine)
        return jnp.stack([even_rows, odd_rows], axis=1).reshape(2 * mine.shape[0], mine.shape[1])

    key_all = in_order(k_rows, k_other).reshape(length, heads_here, HD)
    value_all = in_order(v_rows, v_other).reshape(length, heads_here, HD)
    query_heads = q_rows.reshape(own_rows, heads_here, HD)
    grad_heads = g_rows.reshape(own_rows, heads_here, HD)
    key_total = jnp.zeros((length, heads_here, HD), jnp.float32)
    value_total = jnp.zeros((length, heads_here, HD), jnp.float32)
    query_parts = []
    for block in range(block_count):
        start = block * block_rows
        stop = start + block_rows
        low = 2 * (start // doc_rows * doc_rows)
        high = 2 * stop
        query_block = query_heads[start:stop]
        grad_block = grad_heads[start:stop]
        key_block = key_all[low:high]
        value_block = value_all[low:high]
        scores = (
            jnp.einsum("qhd,khd->hqk", query_block, key_block, preferred_element_type=jnp.float32)
            * scale
        )
        query_pos = 2 * (start + jnp.arange(block_rows, dtype=jnp.int32)) + parity
        key_pos = low + jnp.arange(high - low, dtype=jnp.int32)
        visible = key_pos[None, :] <= query_pos[:, None]
        scores = jnp.where(visible[None], scores, -jnp.inf)
        top = jnp.max(scores, axis=2, keepdims=True)
        weights = jnp.exp(scores - top)
        probs = weights / jnp.sum(weights, axis=2, keepdims=True)
        probs_low = probs.astype(jnp.bfloat16)
        dprob = jnp.einsum(
            "qhd,khd->hqk", grad_block, value_block, preferred_element_type=jnp.float32
        )
        delta = jnp.sum(probs * dprob, axis=2, keepdims=True)
        dscore = (probs * (dprob - delta) * scale).astype(jnp.bfloat16)
        query_parts.append(
            jnp.einsum(
                "hqk,khd->qhd", dscore, key_block, preferred_element_type=jnp.float32
            ).astype(jnp.bfloat16)
        )
        key_total = key_total.at[low:high].add(
            jnp.einsum("hqk,qhd->khd", dscore, query_block, preferred_element_type=jnp.float32)
        )
        value_total = value_total.at[low:high].add(
            jnp.einsum("hqk,qhd->khd", probs_low, grad_block, preferred_element_type=jnp.float32)
        )
    query_grad = jnp.concatenate(query_parts, axis=0).reshape(own_rows, group_width)

    def by_parity(total):
        paired = total.reshape(own_rows, 2, group_width)
        mine = jnp.where(is_even, paired[:, 0], paired[:, 1])
        theirs = jnp.where(is_even, paired[:, 1], paired[:, 0])
        return (mine.astype(jnp.bfloat16), theirs.astype(jnp.bfloat16))

    key_mine, key_theirs = by_parity(key_total)
    value_mine, value_theirs = by_parity(value_total)
    key_back, value_back = partner((key_theirs, value_theirs), "seq", 0)
    key_grad = (key_mine.astype(jnp.float32) + key_back.astype(jnp.float32)).astype(jnp.bfloat16)
    value_grad = (value_mine.astype(jnp.float32) + value_back.astype(jnp.float32)).astype(
        jnp.bfloat16
    )
    spread = jnp.broadcast_to(
        inputs[0].reshape(half_rows, 1, 2, model_width), (half_rows, groups, 2, model_width)
    ).reshape(half_rows, seq_count, model_width)
    input_rows = lax.all_to_all(spread, "seq", split_axis=1, concat_axis=0, tiled=True).reshape(
        own_rows, model_width
    )
    term = jnp.einsum("td,tc->dc", input_rows, value_grad, preferred_element_type=jnp.float32)
    halves = term.reshape(term.shape[0], 2, term.shape[1] // 2)
    mine = jnp.where(is_even, halves[:, 0], halves[:, 1])
    theirs = jnp.where(is_even, halves[:, 1], halves[:, 0])
    mine, theirs = (mine, theirs)
    received = partner(theirs.astype(jnp.bfloat16), "seq", 0).astype(theirs.dtype)
    weight_grad = lax.psum_scatter(
        (mine + received).astype(jnp.bfloat16), "dp", scatter_dimension=0, tiled=True
    ).astype(jnp.float32)

    def to_tokens(array):
        return array.reshape(seq_count, half_rows, 1, group_width)

    def from_heads(array):
        return (
            array.reshape(half_rows, groups, 2, group_width)
            .transpose(0, 2, 1, 3)
            .reshape(1, tok_rows, width)
        )

    returned = (
        lax.all_to_all(to_tokens(query_grad), "seq", split_axis=0, concat_axis=2, tiled=True),
        lax.all_to_all(to_tokens(key_grad), "seq", split_axis=0, concat_axis=2, tiled=True),
        lax.all_to_all(to_tokens(value_grad), "seq", split_axis=0, concat_axis=2, tiled=True),
    )
    return (from_heads(returned[0]), from_heads(returned[1]), from_heads(returned[2]), weight_grad)


def swap(value, axis, bit):
    return lax.ppermute(value, axis, [(i, i ^ bit) for i in range(lax.axis_size(axis))])


def dot(a, b, dims):
    return lax.dot_general(a, b, (dims, ((), ())), preferred_element_type=jnp.float32)


def local_call(kernel, name, outs, scratch=()):
    in_vmem = pl.BlockSpec(memory_space=pltpu.VMEM)

    def call(*operands):
        return pl.pallas_call(
            kernel,
            in_specs=[in_vmem] * len(operands),
            out_specs=[in_vmem] * len(outs),
            out_shape=outs,
            scratch_shapes=scratch,
            compiler_params=pltpu.CompilerParams(vmem_limit_bytes=16 << 20),
            name=name,
        )(*(pltpu.with_memory_space_constraint(a, pltpu.VMEM) for a in operands))

    return call


def columns(start):
    return pl.ds(pl.multiple_of(start * HD, HD), HD)


def both(mine, theirs, group, core, head):
    packed, spread = columns(2 * group + head), columns(4 * group + 2 * core + head)
    own = packed if mine.shape[1] < theirs.shape[1] else spread
    return jnp.concatenate([mine[:, own], theirs[:, spread]], axis=0)


def packed_inputs(arrays, inputs):
    half, width = inputs.shape
    block = inputs.shape[1] // 4
    count = len(arrays)
    groups = width // (4 * HD)

    def kernel(*refs):
        core, sample = lax.axis_index("seq") % 2, lax.axis_index("dp")
        outs, sems = refs[count + 1 : -1], refs[-1]
        copies = []
        for apart, out in enumerate(outs[count:]):
            start = pl.multiple_of((sample ^ apart) * block, block)
            copies.append((refs[count].at[:, pl.ds(start, block)], out))
        for source, out in zip(refs[:count], outs):
            for group in range(groups):
                start = pl.multiple_of((4 * group + 2 * core) * HD, 2 * HD)
                here = slice(2 * group * HD, 2 * (group + 1) * HD)
                copies.append((source.at[:, pl.ds(start, 2 * HD)], out.at[:, here]))
        copies = [pltpu.make_async_copy(a, b, sems.at[i]) for i, (a, b) in enumerate(copies)]
        for copy in copies:
            copy.start()
        for copy in copies:
            copy.wait()

    return pl.pallas_call(
        kernel,
        in_specs=[pl.BlockSpec(memory_space=pl.ANY)] * (count + 1),
        out_specs=[pl.BlockSpec(memory_space=pltpu.VMEM)] * (count + 4),
        out_shape=[pltpu.VMEM((half, width // 2), jnp.bfloat16)] * count
        + [pltpu.VMEM((half, block), jnp.bfloat16)] * 4,
        scratch_shapes=[pltpu.SemaphoreType.DMA((4 + count * groups,))],
        compiler_params=pltpu.CompilerParams(vmem_limit_bytes=16 << 20),
        name="packed_inputs",
    )(*(pltpu.with_memory_space_constraint(a, pltpu.HBM) for a in (*arrays, inputs)))


def probs_by_key(core, queries, keys):
    rows = queries.shape[0]
    scores = dot(keys, queries, ((1,), (1,))) * HD ** (-0.5)
    key_pos = (lax.broadcasted_iota(jnp.int32, (rows, rows), 0) + core * (rows // 2)) & (rows - 1)
    query_pos = (lax.broadcasted_iota(jnp.int32, (rows, rows), 1) + core * (rows // 2)) & (rows - 1)
    scores = jnp.where(key_pos <= query_pos, scores, -jnp.inf)
    weights = jnp.exp(scores - jnp.max(scores, axis=0, keepdims=True))
    return weights * (1.0 / jnp.sum(weights, axis=0, keepdims=True))


def causal_probs(queries, keys, before):
    scores = dot(keys, queries, ((1,), (1,))) * HD ** (-0.5)
    key_pos = lax.broadcasted_iota(jnp.int32, scores.shape, 0)
    query_pos = lax.broadcasted_iota(jnp.int32, scores.shape, 1) + before
    scores = jnp.where(key_pos <= query_pos, scores, -jnp.inf)
    weights = jnp.exp(scores - jnp.max(scores, axis=0, keepdims=True))
    probs = weights * (1.0 / jnp.sum(weights, axis=0, keepdims=True))
    return probs.astype(jnp.bfloat16)


def value_part(q, k, g):
    half, width = q[1].shape
    order = (0, 2, 1, 3)

    def run(core, chip, q0, q1, k0, k1, g0, g1, kept, given):
        for at, apart in enumerate(order):
            for head in range(2):
                group = chip ^ apart
                packed, spread = columns(2 * group + head), columns(4 * group + 2 * core + head)
                mine = [ref[:, packed if ref.shape[1] < width else spread] for ref in (q0, k0, g0)]
                theirs = [ref[:, spread] for ref in (q1, k1, g1)]
                low, high = (theirs, mine) if core else (mine, theirs)
                late = causal_probs(high[0], jnp.concatenate([low[1], high[1]], axis=0), half)
                early = causal_probs(low[0], low[1], 0)
                both_grads = dot(late, high[2], ((1,), (0,)))
                low_grad = both_grads[:half] + dot(early, low[2], ((1,), (0,)))
                here = slice((2 * head + at % 2) * HD, (2 * head + at % 2 + 1) * HD)
                out = (kept, given)[at // 2]
                out[core * half : (core + 1) * half, here] = low_grad.astype(jnp.bfloat16)
                out[(1 - core) * half : (2 - core) * half, here] = both_grads[half:].astype(
                    jnp.bfloat16
                )

    def kernel(*refs):
        chip = lax.axis_index("seq") // 2
        for core in range(2):
            pl.when(lax.axis_index("seq") % 2 == core)(lambda core=core: run(core, chip, *refs))

    out = pltpu.VMEM((2 * half, width // 4), jnp.bfloat16)
    return local_call(kernel, "value_part", [out] * 2)(*q, *k, *g)


def score_part(q, k, v, g):
    half, width = q[1].shape
    heads = width // (2 * HD)

    def kernel(q0, q1, k0, k1, v0, v1, g0, g1, q_mine, q_theirs, k_mine, k_theirs):
        core = lax.axis_index("seq") % 2
        for head in range(heads):
            where = head // 2, core, head % 2
            queries, keys = both(q0, q1, *where), both(k0, k1, *where)
            probs = probs_by_key(core, queries, keys)
            dprob = dot(both(v0, v1, *where), both(g0, g1, *where), ((1,), (1,)))
            delta = jnp.sum(probs * dprob, axis=0, keepdims=True)
            dscore = (probs * (dprob - delta) * HD ** (-0.5)).astype(jnp.bfloat16)
            key_grad = dot(dscore, queries, ((1,), (0,))).astype(jnp.bfloat16)
            query_grad = dot(dscore, keys, ((0,), (0,))).astype(jnp.bfloat16)
            there = slice(head * HD, (head + 1) * HD)
            q_mine[:, there] = query_grad[:half]
            q_theirs[:, there] = query_grad[half:]
            k_mine[:, there] = key_grad[:half]
            k_theirs[:, there] = key_grad[half:]

    out = pltpu.VMEM((half, heads * HD), jnp.bfloat16)
    return local_call(kernel, "score_part", [out] * 4)(*q, *k, *v, *g)


def turned(pieces):
    rows, width = pieces[0].shape

    def kernel(*refs):
        for i, piece in enumerate(refs[:-1]):
            refs[-1][:, i * rows : (i + 1) * rows] = piece[...].T

    out = pltpu.VMEM((width, rows * len(pieces)), jnp.bfloat16)
    return local_call(kernel, "turned", [out])(*pieces)[0]


def term_part(turned_inputs, near, far):
    rows = turned_inputs[0].shape[0]
    width = near[0].shape[1] // 2
    half = near[0].shape[0] // 2
    count = len(near)

    def kernel(*refs):
        outs = refs[-2:]
        total = None
        for i, x_ref in enumerate(refs[:4]):
            values = refs[4 + i // 2 * count : 4 + (i // 2 + 1) * count]
            here = slice(i % 2 * half, (i % 2 + 1) * half)
            part = jnp.concatenate([ref[here, :] for ref in values], axis=0)
            product = dot(x_ref[...], part, ((1,), (0,)))
            total = product if total is None else total + product
        for i, out in enumerate(outs):
            out[...] = total[:, i * width : (i + 1) * width].astype(out.dtype)

    outs = [pltpu.VMEM((rows, width), kind) for kind in (jnp.float32, jnp.bfloat16)]
    return local_call(kernel, "term_part", outs)(*turned_inputs, *near, *far)


def joined(mine, theirs):
    half = mine[0].shape[0]
    width = 2 * mine[0].shape[1]

    def kernel(*refs):
        outs = refs[-3:]
        core, chip = lax.axis_index("seq") % 2, lax.axis_index("seq") // 2
        for ins, owner in ((refs[:4], core), (refs[4:8], 1 - core)):
            for i in range(width // (4 * HD)):
                for j in range(2):
                    where = columns(4 * i + 2 * owner + j)
                    here = slice((2 * i + j) * HD, (2 * i + j + 1) * HD)
                    outs[0][:, where] = ins[0][:, here]
                    outs[1][:, where] = ins[1][:, here]
                    where = columns(4 * (chip ^ i) + 2 * owner + j)
                    here = slice((2 * j + i // 2) * HD, (2 * j + i // 2 + 1) * HD)
                    outs[2][:, where] = ins[2 + i % 2][:, here]

    out = jax.ShapeDtypeStruct((half, width), jnp.bfloat16)
    return local_call(kernel, "joined", [out] * 3)(*mine, *theirs)


def after(values, *earlier):
    return list(lax.optimization_barrier((*values, *earlier))[: len(values)])


def chip_body(queries, key_vectors, values, out_grad, inputs):
    half = queries.shape[1]
    arrays = [a[0] for a in (queries, key_vectors, out_grad, values)]
    *packed, x_here, x_1, x_2, x_3 = packed_inputs([arrays[i] for i in (2,)], inputs[0])
    own = dict(zip((2,), packed))
    q, k, g, v = ((own.get(i, a), swap(a, "seq", 1)) for i, a in enumerate(arrays))
    x_mine = [x_here, swap(x_1, "dp", 1), swap(x_2, "dp", 2), swap(x_3, "dp", 3)]

    kept, given = value_part(q, k, g)
    q_mine, q_theirs, k_mine, k_theirs = score_part(q, k, v, g)
    back = [swap(a, "seq", 1) for a in (q_theirs, k_theirs, kept[half:], given[half:])]
    query_grad, key_grad, value_grad = joined([q_mine, k_mine, kept[:half], given[:half]], back)
    got = swap(given, "seq", 2)
    sides = []
    for head in range(2):
        here = slice(2 * head * HD, 2 * (head + 1) * HD)
        paired = jnp.concatenate([kept[:, here], got[:, here]], axis=0)
        by_x, by_y = after([swap(paired, "dp", 1), swap(paired, "dp", 2)])
        cross = swap(by_x, "dp", 2) if head else swap(by_y, "dp", 1)
        near = [paired[: 2 * half], by_x[: 2 * half], by_y[: 2 * half], cross[: 2 * half]]
        far = [paired[2 * half :], by_x[2 * half :], by_y[2 * half :], cross[2 * half :]]
        sides.append((near, far))

    x_mine = after(x_mine, got, q_theirs)
    x_own = turned(x_mine)
    x_next = swap([x_own][0], "seq", 2)
    x_turned = [x_own, swap(x_own, "seq", 1), x_next, swap(after([x_next], query_grad)[0], "seq", 1)]

    blocks = []
    for near, far in sides:
        mine, sent = term_part(x_turned, near, far)
        blocks.append(mine + swap(sent, "seq", 4).astype(jnp.float32))
    weight_grad = jnp.concatenate(blocks, axis=1)

    return query_grad[None], key_grad[None], value_grad[None], weight_grad


def solution(mesh):
    on_chip = mesh.shape["dp"] == 4 and mesh.shape["seq"] == 8
    return jax.shard_map(
        chip_body if on_chip else body,
        mesh=mesh,
        in_specs=(
            P("dp", "seq", None),
            P("dp", "seq", None),
            P("dp", "seq", None),
            P("dp", "seq", None),
            P("dp", "seq", None),
        ),
        out_specs=(
            P("dp", "seq", None),
            P("dp", "seq", None),
            P("dp", "seq", None),
            P("dp", "seq"),
        ),
        check_vma=False,
    )
```

```python
import jax
import jax.numpy as jnp
from jax import lax
from jax.experimental import pallas as pl
from jax.experimental.pallas import tpu as pltpu
from jax.sharding import PartitionSpec as P

HD = 128


def partner(value, axis, apart):
    return lax.ppermute(value, axis, [(i, i ^ 1 << apart) for i in range(lax.axis_size(axis))])


def body(queries, key_vectors, values, out_grad, inputs):
    seq_count = lax.axis_size("seq")
    groups = seq_count // 2
    parity = lax.axis_index("seq") % 2
    is_even = parity == 0
    tok_rows = queries.shape[1]
    half_rows = tok_rows // 2
    width = queries.shape[2]
    group_width = 2 * width // seq_count
    heads_here = group_width // HD
    model_width = inputs.shape[2]
    own_rows = seq_count * half_rows
    length = 2 * own_rows
    doc_rows = own_rows // 4
    block_rows = min(doc_rows, max(256, length // 16))
    block_count = own_rows // block_rows
    scale = HD ** (-0.5)

    def to_heads(array):
        return (
            array[0]
            .reshape(half_rows, 2, groups, group_width)
            .transpose(0, 2, 1, 3)
            .reshape(half_rows, seq_count, group_width)
        )

    moved = (
        lax.all_to_all(to_heads(queries), "seq", split_axis=1, concat_axis=0, tiled=True),
        lax.all_to_all(to_heads(key_vectors), "seq", split_axis=1, concat_axis=0, tiled=True),
        lax.all_to_all(to_heads(values), "seq", split_axis=1, concat_axis=0, tiled=True),
        lax.all_to_all(to_heads(out_grad), "seq", split_axis=1, concat_axis=0, tiled=True),
    )
    q_rows = moved[0].reshape(own_rows, group_width)
    k_rows = moved[1].reshape(own_rows, group_width)
    v_rows = moved[2].reshape(own_rows, group_width)
    g_rows = moved[3].reshape(own_rows, group_width)
    k_other, v_other = partner((k_rows, v_rows), "seq", 0)

    def in_order(mine, theirs):
        even_rows = jnp.where(is_even, mine, theirs)
        odd_rows = jnp.where(is_even, theirs, mine)
        return jnp.stack([even_rows, odd_rows], axis=1).reshape(2 * mine.shape[0], mine.shape[1])

    key_all = in_order(k_rows, k_other).reshape(length, heads_here, HD)
    value_all = in_order(v_rows, v_other).reshape(length, heads_here, HD)
    query_heads = q_rows.reshape(own_rows, heads_here, HD)
    grad_heads = g_rows.reshape(own_rows, heads_here, HD)
    key_total = jnp.zeros((length, heads_here, HD), jnp.float32)
    value_total = jnp.zeros((length, heads_here, HD), jnp.float32)
    query_parts = []
    for block in range(block_count):
        start = block * block_rows
        stop = start + block_rows
        low = 2 * (start // doc_rows * doc_rows)
        high = 2 * stop
        query_block = query_heads[start:stop]
        grad_block = grad_heads[start:stop]
        key_block = key_all[low:high]
        value_block = value_all[low:high]
        scores = (
            jnp.einsum("qhd,khd->hqk", query_block, key_block, preferred_element_type=jnp.float32)
            * scale
        )
        query_pos = 2 * (start + jnp.arange(block_rows, dtype=jnp.int32)) + parity
        key_pos = low + jnp.arange(high - low, dtype=jnp.int32)
        visible = key_pos[None, :] <= query_pos[:, None]
        scores = jnp.where(visible[None], scores, -jnp.inf)
        top = jnp.max(scores, axis=2, keepdims=True)
        weights = jnp.exp(scores - top)
        probs = weights / jnp.sum(weights, axis=2, keepdims=True)
        probs_low = probs.astype(jnp.bfloat16)
        dprob = jnp.einsum(
            "qhd,khd->hqk", grad_block, value_block, preferred_element_type=jnp.float32
        )
        delta = jnp.sum(probs * dprob, axis=2, keepdims=True)
        dscore = (probs * (dprob - delta) * scale).astype(jnp.bfloat16)
        query_parts.append(
            jnp.einsum(
                "hqk,khd->qhd", dscore, key_block, preferred_element_type=jnp.float32
            ).astype(jnp.bfloat16)
        )
        key_total = key_total.at[low:high].add(
            jnp.einsum("hqk,qhd->khd", dscore, query_block, preferred_element_type=jnp.float32)
        )
        value_total = value_total.at[low:high].add(
            jnp.einsum("hqk,qhd->khd", probs_low, grad_block, preferred_element_type=jnp.float32)
        )
    query_grad = jnp.concatenate(query_parts, axis=0).reshape(own_rows, group_width)

    def by_parity(total):
        paired = total.reshape(own_rows, 2, group_width)
        mine = jnp.where(is_even, paired[:, 0], paired[:, 1])
        theirs = jnp.where(is_even, paired[:, 1], paired[:, 0])
        return (mine.astype(jnp.bfloat16), theirs.astype(jnp.bfloat16))

    key_mine, key_theirs = by_parity(key_total)
    value_mine, value_theirs = by_parity(value_total)
    key_back, value_back = partner((key_theirs, value_theirs), "seq", 0)
    key_grad = (key_mine.astype(jnp.float32) + key_back.astype(jnp.float32)).astype(jnp.bfloat16)
    value_grad = (value_mine.astype(jnp.float32) + value_back.astype(jnp.float32)).astype(
        jnp.bfloat16
    )
    spread = jnp.broadcast_to(
        inputs[0].reshape(half_rows, 1, 2, model_width), (half_rows, groups, 2, model_width)
    ).reshape(half_rows, seq_count, model_width)
    input_rows = lax.all_to_all(spread, "seq", split_axis=1, concat_axis=0, tiled=True).reshape(
        own_rows, model_width
    )
    term = jnp.einsum("td,tc->dc", input_rows, value_grad, preferred_element_type=jnp.float32)
    halves = term.reshape(term.shape[0], 2, term.shape[1] // 2)
    mine = jnp.where(is_even, halves[:, 0], halves[:, 1])
    theirs = jnp.where(is_even, halves[:, 1], halves[:, 0])
    mine, theirs = (mine, theirs)
    received = partner(theirs.astype(jnp.bfloat16), "seq", 0).astype(theirs.dtype)
    weight_grad = lax.psum_scatter(
        (mine + received).astype(jnp.bfloat16), "dp", scatter_dimension=0, tiled=True
    ).astype(jnp.float32)

    def to_tokens(array):
        return array.reshape(seq_count, half_rows, 1, group_width)

    def from_heads(array):
        return (
            array.reshape(half_rows, groups, 2, group_width)
            .transpose(0, 2, 1, 3)
            .reshape(1, tok_rows, width)
        )

    returned = (
        lax.all_to_all(to_tokens(query_grad), "seq", split_axis=0, concat_axis=2, tiled=True),
        lax.all_to_all(to_tokens(key_grad), "seq", split_axis=0, concat_axis=2, tiled=True),
        lax.all_to_all(to_tokens(value_grad), "seq", split_axis=0, concat_axis=2, tiled=True),
    )
    return (from_heads(returned[0]), from_heads(returned[1]), from_heads(returned[2]), weight_grad)


def swap(value, axis, bit):
    return lax.ppermute(value, axis, [(i, i ^ bit) for i in range(lax.axis_size(axis))])


def dot(a, b, dims):
    return lax.dot_general(a, b, (dims, ((), ())), preferred_element_type=jnp.float32)


def local_call(kernel, name, outs, scratch=()):
    in_vmem = pl.BlockSpec(memory_space=pltpu.VMEM)

    def call(*operands):
        return pl.pallas_call(
            kernel,
            in_specs=[in_vmem] * len(operands),
            out_specs=[in_vmem] * len(outs),
            out_shape=outs,
            scratch_shapes=scratch,
            compiler_params=pltpu.CompilerParams(vmem_limit_bytes=16 << 20),
            name=name,
        )(*(pltpu.with_memory_space_constraint(a, pltpu.VMEM) for a in operands))

    return call


def columns(start):
    return pl.ds(pl.multiple_of(start * HD, HD), HD)


def both(mine, theirs, group, core, head):
    packed, spread = columns(2 * group + head), columns(4 * group + 2 * core + head)
    own = packed if mine.shape[1] < theirs.shape[1] else spread
    return jnp.concatenate([mine[:, own], theirs[:, spread]], axis=0)


def packed_inputs(arrays, inputs):
    half, width = inputs.shape
    block = inputs.shape[1] // 4
    count = len(arrays)
    groups = width // (4 * HD)

    def kernel(*refs):
        core, sample = lax.axis_index("seq") % 2, lax.axis_index("dp")
        outs, sems = refs[count + 1 : -1], refs[-1]
        copies = []
        for apart, out in enumerate(outs[count:]):
            start = pl.multiple_of((sample ^ apart) * block, block)
            copies.append((refs[count].at[:, pl.ds(start, block)], out))
        for source, out in zip(refs[:count], outs):
            for group in range(groups):
                start = pl.multiple_of((4 * group + 2 * core) * HD, 2 * HD)
                here = slice(2 * group * HD, 2 * (group + 1) * HD)
                copies.append((source.at[:, pl.ds(start, 2 * HD)], out.at[:, here]))
        copies = [pltpu.make_async_copy(a, b, sems.at[i]) for i, (a, b) in enumerate(copies)]
        for copy in copies:
            copy.start()
        for copy in copies:
            copy.wait()

    return pl.pallas_call(
        kernel,
        in_specs=[pl.BlockSpec(memory_space=pl.ANY)] * (count + 1),
        out_specs=[pl.BlockSpec(memory_space=pltpu.VMEM)] * (count + 4),
        out_shape=[pltpu.VMEM((half, width // 2), jnp.bfloat16)] * count
        + [pltpu.VMEM((half, block), jnp.bfloat16)] * 4,
        scratch_shapes=[pltpu.SemaphoreType.DMA((4 + count * groups,))],
        compiler_params=pltpu.CompilerParams(vmem_limit_bytes=16 << 20),
        name="packed_inputs",
    )(*(pltpu.with_memory_space_constraint(a, pltpu.HBM) for a in (*arrays, inputs)))


def probs_by_key(core, queries, keys):
    rows = queries.shape[0]
    scores = dot(keys, queries, ((1,), (1,))) * HD ** (-0.5)
    key_pos = (lax.broadcasted_iota(jnp.int32, (rows, rows), 0) + core * (rows // 2)) & (rows - 1)
    query_pos = (lax.broadcasted_iota(jnp.int32, (rows, rows), 1) + core * (rows // 2)) & (rows - 1)
    scores = jnp.where(key_pos <= query_pos, scores, -jnp.inf)
    weights = jnp.exp(scores - jnp.max(scores, axis=0, keepdims=True))
    return weights * (1.0 / jnp.sum(weights, axis=0, keepdims=True))


def causal_probs(queries, keys, before):
    scores = dot(keys, queries, ((1,), (1,))) * HD ** (-0.5)
    key_pos = lax.broadcasted_iota(jnp.int32, scores.shape, 0)
    query_pos = lax.broadcasted_iota(jnp.int32, scores.shape, 1) + before
    scores = jnp.where(key_pos <= query_pos, scores, -jnp.inf)
    weights = jnp.exp(scores - jnp.max(scores, axis=0, keepdims=True))
    probs = weights * (1.0 / jnp.sum(weights, axis=0, keepdims=True))
    return probs.astype(jnp.bfloat16)


def value_part(q, k, g):
    half, width = q[1].shape
    order = (0, 2, 1, 3)

    def run(core, chip, q0, q1, k0, k1, g0, g1, kept, given):
        for at, apart in enumerate(order):
            for head in range(2):
                group = chip ^ apart
                packed, spread = columns(2 * group + head), columns(4 * group + 2 * core + head)
                mine = [ref[:, packed if ref.shape[1] < width else spread] for ref in (q0, k0, g0)]
                theirs = [ref[:, spread] for ref in (q1, k1, g1)]
                low, high = (theirs, mine) if core else (mine, theirs)
                late = causal_probs(high[0], jnp.concatenate([low[1], high[1]], axis=0), half)
                early = causal_probs(low[0], low[1], 0)
                both_grads = dot(late, high[2], ((1,), (0,)))
                low_grad = both_grads[:half] + dot(early, low[2], ((1,), (0,)))
                here = slice((2 * head + at % 2) * HD, (2 * head + at % 2 + 1) * HD)
                out = (kept, given)[at // 2]
                out[core * half : (core + 1) * half, here] = low_grad.astype(jnp.bfloat16)
                out[(1 - core) * half : (2 - core) * half, here] = both_grads[half:].astype(
                    jnp.bfloat16
                )

    def kernel(*refs):
        chip = lax.axis_index("seq") // 2
        for core in range(2):
            pl.when(lax.axis_index("seq") % 2 == core)(lambda core=core: run(core, chip, *refs))

    out = pltpu.VMEM((2 * half, width // 4), jnp.bfloat16)
    return local_call(kernel, "value_part", [out] * 2)(*q, *k, *g)


def score_part(q, k, v, g):
    half, width = q[1].shape
    heads = width // (2 * HD)

    def kernel(q0, q1, k0, k1, v0, v1, g0, g1, q_mine, q_theirs, k_mine, k_theirs):
        core = lax.axis_index("seq") % 2
        for head in range(heads):
            where = head // 2, core, head % 2
            queries, keys = both(q0, q1, *where), both(k0, k1, *where)
            probs = probs_by_key(core, queries, keys)
            dprob = dot(both(v0, v1, *where), both(g0, g1, *where), ((1,), (1,)))
            delta = jnp.sum(probs * dprob, axis=0, keepdims=True)
            dscore = (probs * (dprob - delta) * HD ** (-0.5)).astype(jnp.bfloat16)
            key_grad = dot(dscore, queries, ((1,), (0,))).astype(jnp.bfloat16)
            query_grad = dot(dscore, keys, ((0,), (0,))).astype(jnp.bfloat16)
            there = slice(head * HD, (head + 1) * HD)
            q_mine[:, there] = query_grad[:half]
            q_theirs[:, there] = query_grad[half:]
            k_mine[:, there] = key_grad[:half]
            k_theirs[:, there] = key_grad[half:]

    out = pltpu.VMEM((half, heads * HD), jnp.bfloat16)
    return local_call(kernel, "score_part", [out] * 4)(*q, *k, *v, *g)


def turned(pieces):
    rows, width = pieces[0].shape

    def kernel(*refs):
        for i, piece in enumerate(refs[:-1]):
            refs[-1][:, i * rows : (i + 1) * rows] = piece[...].T

    out = pltpu.VMEM((width, rows * len(pieces)), jnp.bfloat16)
    return local_call(kernel, "turned", [out])(*pieces)[0]


def term_part(turned_inputs, near, far):
    rows = turned_inputs[0].shape[0]
    width = near[0].shape[1] // 2
    half = near[0].shape[0] // 2
    count = len(near)

    def kernel(*refs):
        outs = refs[-2:]
        total = None
        for i, x_ref in enumerate(refs[:4]):
            values = refs[4 + i // 2 * count : 4 + (i // 2 + 1) * count]
            here = slice(i % 2 * half, (i % 2 + 1) * half)
            part = jnp.concatenate([ref[here, :] for ref in values], axis=0)
            product = dot(x_ref[...], part, ((1,), (0,)))
            total = product if total is None else total + product
        for i, out in enumerate(outs):
            out[...] = total[:, i * width : (i + 1) * width].astype(out.dtype)

    outs = [pltpu.VMEM((rows, width), kind) for kind in (jnp.float32, jnp.bfloat16)]
    return local_call(kernel, "term_part", outs)(*turned_inputs, *near, *far)


def joined(mine, theirs):
    half = mine[0].shape[0]
    width = 2 * mine[0].shape[1]

    def kernel(*refs):
        outs = refs[-3:]
        core, chip = lax.axis_index("seq") % 2, lax.axis_index("seq") // 2
        for ins, owner in ((refs[:4], core), (refs[4:8], 1 - core)):
            for i in range(width // (4 * HD)):
                for j in range(2):
                    where = columns(4 * i + 2 * owner + j)
                    here = slice((2 * i + j) * HD, (2 * i + j + 1) * HD)
                    outs[0][:, where] = ins[0][:, here]
                    outs[1][:, where] = ins[1][:, here]
                    where = columns(4 * (chip ^ i) + 2 * owner + j)
                    here = slice((2 * j + i // 2) * HD, (2 * j + i // 2 + 1) * HD)
                    outs[2][:, where] = ins[2 + i % 2][:, here]

    out = jax.ShapeDtypeStruct((half, width), jnp.bfloat16)
    return local_call(kernel, "joined", [out] * 3)(*mine, *theirs)


def after(values, *earlier):
    return list(lax.optimization_barrier((*values, *earlier))[: len(values)])


def chip_body(queries, key_vectors, values, out_grad, inputs):
    half = queries.shape[1]
    arrays = [a[0] for a in (queries, key_vectors, out_grad, values)]
    *packed, x_here, x_1, x_2, x_3 = packed_inputs([arrays[i] for i in (2,)], inputs[0])
    own = dict(zip((2,), packed))
    q, k, g, v = ((own.get(i, a), swap(a, "seq", 1)) for i, a in enumerate(arrays))
    x_mine = [x_here, swap(x_1, "dp", 1), swap(x_2, "dp", 2), swap(x_3, "dp", 3)]

    kept, given = value_part(q, k, g)
    q_mine, q_theirs, k_mine, k_theirs = score_part(q, k, v, g)
    back = [swap(a, "seq", 1) for a in (q_theirs, k_theirs, kept[half:], given[half:])]
    query_grad, key_grad, value_grad = joined([q_mine, k_mine, kept[:half], given[:half]], back)
    got = swap(given, "seq", 2)
    sides = []
    for head in range(2):
        here = slice(2 * head * HD, 2 * (head + 1) * HD)
        paired = jnp.concatenate([kept[:, here], got[:, here]], axis=0)
        by_x, by_y = after([swap(paired, "dp", 1), swap(paired, "dp", 2)])
        first, second = after([swap(by_y[: 2 * half], "dp", 1), swap(by_x[2 * half :], "dp", 2)])
        near = [paired[: 2 * half], by_x[: 2 * half], by_y[: 2 * half], first]
        far = [paired[2 * half :], by_x[2 * half :], by_y[2 * half :], second]
        sides.append((near, far))

    x_mine = after(x_mine, got, q_theirs)
    x_own = turned(x_mine)
    x_next = swap([x_own][0], "seq", 2)
    x_turned = [x_own, swap(x_own, "seq", 1), x_next, swap(after([x_next], query_grad)[0], "seq", 1)]

    blocks = []
    for near, far in sides:
        mine, sent = term_part(x_turned, near, far)
        blocks.append(mine + swap(sent, "seq", 4).astype(jnp.float32))
    weight_grad = jnp.concatenate(blocks, axis=1)

    return query_grad[None], key_grad[None], value_grad[None], weight_grad


def solution(mesh):
    on_chip = mesh.shape["dp"] == 4 and mesh.shape["seq"] == 8
    return jax.shard_map(
        chip_body if on_chip else body,
        mesh=mesh,
        in_specs=(
            P("dp", "seq", None),
            P("dp", "seq", None),
            P("dp", "seq", None),
            P("dp", "seq", None),
            P("dp", "seq", None),
        ),
        out_specs=(
            P("dp", "seq", None),
            P("dp", "seq", None),
            P("dp", "seq", None),
            P("dp", "seq"),
        ),
        check_vma=False,
    )
```

```python
import jax
import jax.numpy as jnp
from jax import lax
from jax.experimental import pallas as pl
from jax.experimental.pallas import tpu as pltpu
from jax.sharding import PartitionSpec as P

HD = 128


def partner(value, axis, apart):
    return lax.ppermute(value, axis, [(i, i ^ 1 << apart) for i in range(lax.axis_size(axis))])


def body(queries, key_vectors, values, out_grad, inputs):
    seq_count = lax.axis_size("seq")
    groups = seq_count // 2
    parity = lax.axis_index("seq") % 2
    is_even = parity == 0
    tok_rows = queries.shape[1]
    half_rows = tok_rows // 2
    width = queries.shape[2]
    group_width = 2 * width // seq_count
    heads_here = group_width // HD
    model_width = inputs.shape[2]
    own_rows = seq_count * half_rows
    length = 2 * own_rows
    doc_rows = own_rows // 4
    block_rows = min(doc_rows, max(256, length // 16))
    block_count = own_rows // block_rows
    scale = HD ** (-0.5)

    def to_heads(array):
        return (
            array[0]
            .reshape(half_rows, 2, groups, group_width)
            .transpose(0, 2, 1, 3)
            .reshape(half_rows, seq_count, group_width)
        )

    moved = (
        lax.all_to_all(to_heads(queries), "seq", split_axis=1, concat_axis=0, tiled=True),
        lax.all_to_all(to_heads(key_vectors), "seq", split_axis=1, concat_axis=0, tiled=True),
        lax.all_to_all(to_heads(values), "seq", split_axis=1, concat_axis=0, tiled=True),
        lax.all_to_all(to_heads(out_grad), "seq", split_axis=1, concat_axis=0, tiled=True),
    )
    q_rows = moved[0].reshape(own_rows, group_width)
    k_rows = moved[1].reshape(own_rows, group_width)
    v_rows = moved[2].reshape(own_rows, group_width)
    g_rows = moved[3].reshape(own_rows, group_width)
    k_other, v_other = partner((k_rows, v_rows), "seq", 0)

    def in_order(mine, theirs):
        even_rows = jnp.where(is_even, mine, theirs)
        odd_rows = jnp.where(is_even, theirs, mine)
        return jnp.stack([even_rows, odd_rows], axis=1).reshape(2 * mine.shape[0], mine.shape[1])

    key_all = in_order(k_rows, k_other).reshape(length, heads_here, HD)
    value_all = in_order(v_rows, v_other).reshape(length, heads_here, HD)
    query_heads = q_rows.reshape(own_rows, heads_here, HD)
    grad_heads = g_rows.reshape(own_rows, heads_here, HD)
    key_total = jnp.zeros((length, heads_here, HD), jnp.float32)
    value_total = jnp.zeros((length, heads_here, HD), jnp.float32)
    query_parts = []
    for block in range(block_count):
        start = block * block_rows
        stop = start + block_rows
        low = 2 * (start // doc_rows * doc_rows)
        high = 2 * stop
        query_block = query_heads[start:stop]
        grad_block = grad_heads[start:stop]
        key_block = key_all[low:high]
        value_block = value_all[low:high]
        scores = (
            jnp.einsum("qhd,khd->hqk", query_block, key_block, preferred_element_type=jnp.float32)
            * scale
        )
        query_pos = 2 * (start + jnp.arange(block_rows, dtype=jnp.int32)) + parity
        key_pos = low + jnp.arange(high - low, dtype=jnp.int32)
        visible = key_pos[None, :] <= query_pos[:, None]
        scores = jnp.where(visible[None], scores, -jnp.inf)
        top = jnp.max(scores, axis=2, keepdims=True)
        weights = jnp.exp(scores - top)
        probs = weights / jnp.sum(weights, axis=2, keepdims=True)
        probs_low = probs.astype(jnp.bfloat16)
        dprob = jnp.einsum(
            "qhd,khd->hqk", grad_block, value_block, preferred_element_type=jnp.float32
        )
        delta = jnp.sum(probs * dprob, axis=2, keepdims=True)
        dscore = (probs * (dprob - delta) * scale).astype(jnp.bfloat16)
        query_parts.append(
            jnp.einsum(
                "hqk,khd->qhd", dscore, key_block, preferred_element_type=jnp.float32
            ).astype(jnp.bfloat16)
        )
        key_total = key_total.at[low:high].add(
            jnp.einsum("hqk,qhd->khd", dscore, query_block, preferred_element_type=jnp.float32)
        )
        value_total = value_total.at[low:high].add(
            jnp.einsum("hqk,qhd->khd", probs_low, grad_block, preferred_element_type=jnp.float32)
        )
    query_grad = jnp.concatenate(query_parts, axis=0).reshape(own_rows, group_width)

    def by_parity(total):
        paired = total.reshape(own_rows, 2, group_width)
        mine = jnp.where(is_even, paired[:, 0], paired[:, 1])
        theirs = jnp.where(is_even, paired[:, 1], paired[:, 0])
        return (mine.astype(jnp.bfloat16), theirs.astype(jnp.bfloat16))

    key_mine, key_theirs = by_parity(key_total)
    value_mine, value_theirs = by_parity(value_total)
    key_back, value_back = partner((key_theirs, value_theirs), "seq", 0)
    key_grad = (key_mine.astype(jnp.float32) + key_back.astype(jnp.float32)).astype(jnp.bfloat16)
    value_grad = (value_mine.astype(jnp.float32) + value_back.astype(jnp.float32)).astype(
        jnp.bfloat16
    )
    spread = jnp.broadcast_to(
        inputs[0].reshape(half_rows, 1, 2, model_width), (half_rows, groups, 2, model_width)
    ).reshape(half_rows, seq_count, model_width)
    input_rows = lax.all_to_all(spread, "seq", split_axis=1, concat_axis=0, tiled=True).reshape(
        own_rows, model_width
    )
    term = jnp.einsum("td,tc->dc", input_rows, value_grad, preferred_element_type=jnp.float32)
    halves = term.reshape(term.shape[0], 2, term.shape[1] // 2)
    mine = jnp.where(is_even, halves[:, 0], halves[:, 1])
    theirs = jnp.where(is_even, halves[:, 1], halves[:, 0])
    mine, theirs = (mine, theirs)
    received = partner(theirs.astype(jnp.bfloat16), "seq", 0).astype(theirs.dtype)
    weight_grad = lax.psum_scatter(
        (mine + received).astype(jnp.bfloat16), "dp", scatter_dimension=0, tiled=True
    ).astype(jnp.float32)

    def to_tokens(array):
        return array.reshape(seq_count, half_rows, 1, group_width)

    def from_heads(array):
        return (
            array.reshape(half_rows, groups, 2, group_width)
            .transpose(0, 2, 1, 3)
            .reshape(1, tok_rows, width)
        )

    returned = (
        lax.all_to_all(to_tokens(query_grad), "seq", split_axis=0, concat_axis=2, tiled=True),
        lax.all_to_all(to_tokens(key_grad), "seq", split_axis=0, concat_axis=2, tiled=True),
        lax.all_to_all(to_tokens(value_grad), "seq", split_axis=0, concat_axis=2, tiled=True),
    )
    return (from_heads(returned[0]), from_heads(returned[1]), from_heads(returned[2]), weight_grad)


def swap(value, axis, bit):
    return lax.ppermute(value, axis, [(i, i ^ bit) for i in range(lax.axis_size(axis))])


def dot(a, b, dims):
    return lax.dot_general(a, b, (dims, ((), ())), preferred_element_type=jnp.float32)


def local_call(kernel, name, outs, scratch=()):
    in_vmem = pl.BlockSpec(memory_space=pltpu.VMEM)

    def call(*operands):
        return pl.pallas_call(
            kernel,
            in_specs=[in_vmem] * len(operands),
            out_specs=[in_vmem] * len(outs),
            out_shape=outs,
            scratch_shapes=scratch,
            compiler_params=pltpu.CompilerParams(vmem_limit_bytes=16 << 20),
            name=name,
        )(*(pltpu.with_memory_space_constraint(a, pltpu.VMEM) for a in operands))

    return call


def columns(start):
    return pl.ds(pl.multiple_of(start * HD, HD), HD)


def both(mine, theirs, group, core, head):
    packed, spread = columns(2 * group + head), columns(4 * group + 2 * core + head)
    return jnp.concatenate([mine[:, packed], theirs[:, spread]], axis=0)


def packed_inputs(arrays, inputs):
    half, width = arrays[0].shape
    block = inputs.shape[1] // 4
    count = len(arrays)
    groups = width // (4 * HD)

    def kernel(*refs):
        core, sample = lax.axis_index("seq") % 2, lax.axis_index("dp")
        outs, sems = refs[count + 1 : -1], refs[-1]
        copies = []
        for apart, out in enumerate(outs[count:]):
            start = pl.multiple_of((sample ^ apart) * block, block)
            copies.append((refs[count].at[:, pl.ds(start, block)], out))
        for source, out in zip(refs[:count], outs):
            for group in range(groups):
                start = pl.multiple_of((4 * group + 2 * core) * HD, 2 * HD)
                here = slice(2 * group * HD, 2 * (group + 1) * HD)
                copies.append((source.at[:, pl.ds(start, 2 * HD)], out.at[:, here]))
        copies = [pltpu.make_async_copy(a, b, sems.at[i]) for i, (a, b) in enumerate(copies)]
        for copy in copies:
            copy.start()
        for copy in copies:
            copy.wait()

    return pl.pallas_call(
        kernel,
        in_specs=[pl.BlockSpec(memory_space=pl.ANY)] * (count + 1),
        out_specs=[pl.BlockSpec(memory_space=pltpu.VMEM)] * (count + 4),
        out_shape=[pltpu.VMEM((half, width // 2), jnp.bfloat16)] * count
        + [pltpu.VMEM((half, block), jnp.bfloat16)] * 4,
        scratch_shapes=[pltpu.SemaphoreType.DMA((4 + count * groups,))],
        compiler_params=pltpu.CompilerParams(vmem_limit_bytes=16 << 20),
        name="packed_inputs",
    )(*(pltpu.with_memory_space_constraint(a, pltpu.HBM) for a in (*arrays, inputs)))


def probs_by_key(core, queries, keys):
    rows = queries.shape[0]
    scores = dot(keys, queries, ((1,), (1,))) * HD ** (-0.5)
    key_pos = (lax.broadcasted_iota(jnp.int32, (rows, rows), 0) + core * (rows // 2)) & (rows - 1)
    query_pos = (lax.broadcasted_iota(jnp.int32, (rows, rows), 1) + core * (rows // 2)) & (rows - 1)
    scores = jnp.where(key_pos <= query_pos, scores, -jnp.inf)
    weights = jnp.exp(scores - jnp.max(scores, axis=0, keepdims=True))
    return weights * (1.0 / jnp.sum(weights, axis=0, keepdims=True))


def causal_probs(queries, keys, before):
    scores = dot(keys, queries, ((1,), (1,))) * HD ** (-0.5)
    key_pos = lax.broadcasted_iota(jnp.int32, scores.shape, 0)
    query_pos = lax.broadcasted_iota(jnp.int32, scores.shape, 1) + before
    scores = jnp.where(key_pos <= query_pos, scores, -jnp.inf)
    weights = jnp.exp(scores - jnp.max(scores, axis=0, keepdims=True))
    probs = weights * (1.0 / jnp.sum(weights, axis=0, keepdims=True))
    return probs.astype(jnp.bfloat16)


def value_part(q, k, g):
    half, width = q[1].shape
    order = (0, 2, 1, 3)

    def run(core, chip, q0, q1, k0, k1, g0, g1, kept, given):
        for at, apart in enumerate(order):
            for head in range(2):
                group = chip ^ apart
                packed, spread = columns(2 * group + head), columns(4 * group + 2 * core + head)
                mine = [ref[:, packed] for ref in (q0, k0, g0)]
                theirs = [ref[:, spread] for ref in (q1, k1, g1)]
                low, high = (theirs, mine) if core else (mine, theirs)
                late = causal_probs(high[0], jnp.concatenate([low[1], high[1]], axis=0), half)
                early = causal_probs(low[0], low[1], 0)
                both_grads = dot(late, high[2], ((1,), (0,)))
                low_grad = both_grads[:half] + dot(early, low[2], ((1,), (0,)))
                here = slice((2 * head + at % 2) * HD, (2 * head + at % 2 + 1) * HD)
                out = (kept, given)[at // 2]
                out[core * half : (core + 1) * half, here] = low_grad.astype(jnp.bfloat16)
                out[(1 - core) * half : (2 - core) * half, here] = both_grads[half:].astype(
                    jnp.bfloat16
                )

    def kernel(*refs):
        chip = lax.axis_index("seq") // 2
        for core in range(2):
            pl.when(lax.axis_index("seq") % 2 == core)(lambda core=core: run(core, chip, *refs))

    out = pltpu.VMEM((2 * half, width // 4), jnp.bfloat16)
    return local_call(kernel, "value_part", [out] * 2)(*q, *k, *g)


def score_part(q, k, v, g):
    half, width = q[1].shape
    heads = width // (2 * HD)

    def kernel(q0, q1, k0, k1, v0, v1, g0, g1, q_mine, q_theirs, k_mine, k_theirs):
        core = lax.axis_index("seq") % 2
        for head in range(heads):
            where = head // 2, core, head % 2
            queries, keys = both(q0, q1, *where), both(k0, k1, *where)
            spread = columns(4 * (head // 2) + 2 * core + head % 2)
            values = jnp.concatenate([v0[:, spread], v1[:, spread]], axis=0)
            probs = probs_by_key(core, queries, keys)
            dprob = dot(values, both(g0, g1, *where), ((1,), (1,)))
            delta = jnp.sum(probs * dprob, axis=0, keepdims=True)
            dscore = (probs * (dprob - delta) * HD ** (-0.5)).astype(jnp.bfloat16)
            key_grad = dot(dscore, queries, ((1,), (0,))).astype(jnp.bfloat16)
            query_grad = dot(dscore, keys, ((0,), (0,))).astype(jnp.bfloat16)
            there = slice(head * HD, (head + 1) * HD)
            q_mine[:, there] = query_grad[:half]
            q_theirs[:, there] = query_grad[half:]
            k_mine[:, there] = key_grad[:half]
            k_theirs[:, there] = key_grad[half:]

    out = pltpu.VMEM((half, heads * HD), jnp.bfloat16)
    return local_call(kernel, "score_part", [out] * 4)(*q, *k, *v, *g)


def turned(pieces):
    rows, width = pieces[0].shape

    def kernel(*refs):
        for i, piece in enumerate(refs[:-1]):
            refs[-1][:, i * rows : (i + 1) * rows] = piece[...].T

    out = pltpu.VMEM((width, rows * len(pieces)), jnp.bfloat16)
    return local_call(kernel, "turned", [out])(*pieces)[0]


def term_part(turned_inputs, near, far):
    rows = turned_inputs[0].shape[0]
    width = near[0].shape[1] // 2
    half = near[0].shape[0] // 2
    count = len(near)

    def kernel(*refs):
        outs = refs[-2:]
        total = None
        for i, x_ref in enumerate(refs[:4]):
            values = refs[4 + i // 2 * count : 4 + (i // 2 + 1) * count]
            here = slice(i % 2 * half, (i % 2 + 1) * half)
            part = jnp.concatenate([ref[here, :] for ref in values], axis=0)
            product = dot(x_ref[...], part, ((1,), (0,)))
            total = product if total is None else total + product
        for i, out in enumerate(outs):
            out[...] = total[:, i * width : (i + 1) * width].astype(out.dtype)

    outs = [pltpu.VMEM((rows, width), kind) for kind in (jnp.float32, jnp.bfloat16)]
    return local_call(kernel, "term_part", outs)(*turned_inputs, *near, *far)


def joined(mine, theirs):
    half = mine[0].shape[0]
    width = 2 * mine[0].shape[1]

    def kernel(*refs):
        outs = refs[-3:]
        core, chip = lax.axis_index("seq") % 2, lax.axis_index("seq") // 2
        for ins, owner in ((refs[:4], core), (refs[4:8], 1 - core)):
            for i in range(width // (4 * HD)):
                for j in range(2):
                    where = columns(4 * i + 2 * owner + j)
                    here = slice((2 * i + j) * HD, (2 * i + j + 1) * HD)
                    outs[0][:, where] = ins[0][:, here]
                    outs[1][:, where] = ins[1][:, here]
                    where = columns(4 * (chip ^ i) + 2 * owner + j)
                    here = slice((2 * j + i // 2) * HD, (2 * j + i // 2 + 1) * HD)
                    outs[2][:, where] = ins[2 + i % 2][:, here]

    out = jax.ShapeDtypeStruct((half, width), jnp.bfloat16)
    return local_call(kernel, "joined", [out] * 3)(*mine, *theirs)


def after(values, *earlier):
    return list(lax.optimization_barrier((*values, *earlier))[: len(values)])


def chip_body(queries, key_vectors, values, out_grad, inputs):
    half = queries.shape[1]
    arrays = [a[0] for a in (queries, key_vectors, out_grad, values)]
    *own, x_here, x_1, x_2, x_3 = packed_inputs(arrays[:3], inputs[0])
    q, k, g, v = ((mine, swap(a, "seq", 1)) for mine, a in zip((*own, arrays[3]), arrays))
    x_mine = [x_here, swap(x_1, "dp", 1), swap(x_2, "dp", 2), swap(x_3, "dp", 3)]

    kept, given = value_part(q, k, g)
    q_mine, q_theirs, k_mine, k_theirs = score_part(q, k, v, g)
    back = [swap(a, "seq", 1) for a in (q_theirs, k_theirs, kept[half:], given[half:])]
    query_grad, key_grad, value_grad = joined([q_mine, k_mine, kept[:half], given[:half]], back)
    got = swap(given, "seq", 2)
    sides = []
    for head in range(2):
        here = slice(2 * head * HD, 2 * (head + 1) * HD)
        paired = jnp.concatenate([kept[:, here], got[:, here]], axis=0)
        by_x, by_y = after([swap(paired, "dp", 1), swap(paired, "dp", 2)])
        first, second = after([swap(by_y[: 2 * half], "dp", 1), swap(by_x[2 * half :], "dp", 2)])
        near = [paired[: 2 * half], by_x[: 2 * half], by_y[: 2 * half], first]
        far = [paired[2 * half :], by_x[2 * half :], by_y[2 * half :], second]
        sides.append((near, far))

    x_mine = after(x_mine, got, q_theirs)
    x_own = turned(x_mine)
    x_next = swap([x_own][0], "seq", 2)
    x_turned = [x_own, swap(x_own, "seq", 1), x_next, swap(after([x_next], query_grad)[0], "seq", 1)]

    blocks = []
    for near, far in sides:
        mine, sent = term_part(x_turned, near, far)
        blocks.append(mine + swap(sent, "seq", 4).astype(jnp.float32))
    weight_grad = jnp.concatenate(blocks, axis=1)

    return query_grad[None], key_grad[None], value_grad[None], weight_grad


def solution(mesh):
    on_chip = mesh.shape["dp"] == 4 and mesh.shape["seq"] == 8
    return jax.shard_map(
        chip_body if on_chip else body,
        mesh=mesh,
        in_specs=(
            P("dp", "seq", None),
            P("dp", "seq", None),
            P("dp", "seq", None),
            P("dp", "seq", None),
            P("dp", "seq", None),
        ),
        out_specs=(
            P("dp", "seq", None),
            P("dp", "seq", None),
            P("dp", "seq", None),
            P("dp", "seq"),
        ),
        check_vma=False,
    )
```
